32 devices in a mesh: cond: 2 (over x), gx: 4 (over y, core), yz: 4 (over z).
Axes of the slice: x: 2, y: 2, z: 4, core: 2. Of those that a mesh axis runs over, the one named last changes fastest.
Arguments:
- adjoint: float32 [2, 5, 32, 64, 256], P('cond', None, 'gx', 'yz'), may hold values from -6 to 6
- objective_gradient: float32 [2, 5, 32, 64, 256], P('cond', None, 'gx', 'yz'), may hold values from -6 to 6
- diagonal: float32 [32, 64, 256], P('gx', 'yz'), may hold values from 4 to 12
- flux_blocks: float32 [2, 6, 5, 5], P('cond'), may hold values from -1 to 1
- flux_sensitivity: bfloat16 [2, 5, 32, 64, 256], P('cond', None, 'gx', 'yz'), may hold values from -6 to 6
- surface_mask: int32 [32, 64, 256], P('gx', 'yz'), may hold values 0 or 1
- patch_band_slot: int32 [32, 64], P('gx', 'yz'), may hold values from 0 to 62
- design_basis: float32 [256, 128], replicated, may hold values from -0.046875 to 0.046875
- condition_weights: int32 [2], replicated, may hold values from 1 to 999, as said below
Outputs:
- smoothed: float32 [2, 5, 32, 64, 256], P('cond', None, 'gx', 'yz')
- residual: float32 [2, 5, 32, 64, 256], P('cond', None, 'gx', 'yz')
- design_gradient: float32 [4096], P(('gx', 'yz'))
The draws below stay inside these ranges and needn't reach their ends.
Inputs may be any that keep to these rules, and one draw needn't show every extreme that they name: `condition_weights`: positive integer weights; one condition has weight 999.
All inputs are finite; a program needn't handle non-finite values. No bound on the sum of `surface_mask` on one device may be relied on, other than what follows from the above.
Results may differ from the reference program's by a relative error of at most 0.0003.
Values sent between devices are 32-bit elements; how exact they have to be, the bound alone decides.
A program may use at most 64 MiB of HBM per device.

```python
import math
import jax
import jax.numpy as jnp
import numpy as np
from jax import lax

NZ = 256
NVAR = 5
BAND = 128
BAND_SLOTS = 63
COND = 2
CELLS_FIRST = 32
CELLS_SECOND = 64


def draw_condition_weights(key, part):
    drawn = jax.random.randint(jax.random.fold_in(key, 7), (COND,), 1, 1000, dtype=jnp.int32)
    chosen = jax.random.randint(jax.random.fold_in(key, 8), (), 0, COND, dtype=jnp.int32)
    return jnp.where(jnp.arange(COND, dtype=jnp.int32) == chosen, jnp.int32(999), drawn)


def touch_ends(array, own_key, least, top_value):
    longest = array.shape.index(max(array.shape))
    spots = []
    for shift in (0, 1):
        where = [jax.random.randint(jax.random.fold_in(own_key, axis), (), 0, length) for axis, length in enumerate(array.shape)]
        where[longest] = (where[longest] + shift) % array.shape[longest]
        spots.append(tuple(where))
    return array.at[spots[0]].set(least).at[spots[1]].set(top_value)


def level_of(stream_key, dims, cuts, low, high):
    level = 1.0
    for dim, blocks in cuts:
        steps = jax.random.uniform(jax.random.fold_in(jax.random.fold_in(stream_key, 6), dim), (blocks,), jnp.float32, low / len(cuts), high / len(cuts))
        level = level * jnp.repeat(jnp.exp(steps), dims[dim] // blocks).reshape((-1,) + (1,) * (len(dims) - 1 - dim))
    return level


def rank_table(count, skew):
    loads = [(1 << 20) // math.isqrt(grade ** skew) + 1 for grade in range(1, count + 1)]
    scale = 1 + sum(loads) // (1 << 30)
    return np.cumsum(np.array([max(1, weight // scale) for weight in loads]))


def ranked(own_key, extent, amount, lean):
    grid = rank_table(amount, lean)
    lot = jax.random.randint(jax.random.fold_in(own_key, 1), extent, 0, int(grid[amount - 1]))
    grade = jnp.searchsorted(jnp.asarray(grid, jnp.int32), lot, side="right")
    return jax.random.permutation(jax.random.fold_in(own_key, 2), amount)[grade].astype(jnp.int32)


def centred(key, shape, width, limit, pieces=(), kind=jnp.bfloat16):
    values = width * jax.random.normal(key, shape, jnp.float32)
    if pieces:
        values = values * level_of(key, shape, pieces, -0.22, 0.18)
    return jnp.clip(values, -limit, limit).astype(kind)


def setup_inputs(seed: int = 0) -> dict:
    streams_of = jax.random.split(jax.random.key(seed), 10)
    return {
        "adjoint": centred(streams_of[0], (COND, NVAR, CELLS_FIRST, CELLS_SECOND, NZ), 1.0, 6.0, ((0, 2), (2, 4), (3, 4)), jnp.float32),
        "objective_gradient": centred(streams_of[1], (COND, NVAR, CELLS_FIRST, CELLS_SECOND, NZ), 1.0, 6.0, ((0, 2), (2, 4), (3, 4)), jnp.float32),
        "diagonal": jnp.clip(jnp.exp(math.log(12.0) - 1.0986123 * jax.random.uniform(streams_of[2], (CELLS_FIRST, CELLS_SECOND, NZ), jnp.float32) ** level_of(streams_of[2], (CELLS_FIRST, CELLS_SECOND, NZ), ((0, 4), (1, 4)), -0.2, 0.2)), 4.0, 12.0),
        "flux_blocks": centred(streams_of[3], (COND, 6, NVAR, NVAR), (6 * NVAR) ** -0.5, 1.0, ((0, 2),), jnp.float32),
        "flux_sensitivity": centred(streams_of[4], (COND, NVAR, CELLS_FIRST, CELLS_SECOND, NZ), 1.0, 6.0, ((0, 2), (2, 4), (3, 4))),
        "surface_mask": touch_ends((jax.random.randint(streams_of[5], (CELLS_FIRST, CELLS_SECOND, NZ), 0, 4) < 1).astype(jnp.int32), jax.random.fold_in(streams_of[5], 1), 0, 1),
        "patch_band_slot": touch_ends(ranked(streams_of[6], (CELLS_FIRST, CELLS_SECOND), BAND_SLOTS, 2), jax.random.fold_in(streams_of[6], 3), 0, BAND_SLOTS - 1).astype(jnp.int32),
        "design_basis": centred(streams_of[7], (NZ, BAND), (NZ * CELLS_FIRST * CELLS_SECOND // 32) ** -0.5, 0.046875, (), jnp.float32),
        "condition_weights": draw_condition_weights(jax.random.fold_in(streams_of[9], 71), 0),
    }


relaxation = 0.8
neighbour_starts = ((2, 1, 1), (0, 1, 1), (1, 2, 1), (1, 0, 1), (1, 1, 2), (1, 1, 0))


def apply_operator(padded_field, diagonal, blocks):
    size_x = padded_field.shape[1] - 2
    size_y = padded_field.shape[2] - 2
    size_z = padded_field.shape[3] - 2
    result = diagonal * padded_field[:, 1:-1, 1:-1, 1:-1]
    for direction in range(6):
        start_x, start_y, start_z = neighbour_starts[direction]
        shifted = padded_field[:, start_x:start_x + size_x, start_y:start_y + size_y, start_z:start_z + size_z]
        result = result - jnp.einsum("ec,exyz->cxyz", blocks[direction], shifted, precision=lax.Precision.HIGHEST)
    return result


def spread_bands(slot_lookup):
    halfway = slot_lookup.shape[1] // 2
    first_half = jnp.pad(slot_lookup[:, :halfway], ((0, 1), (0, 0)))
    second_half = jnp.pad(slot_lookup[:, halfway:], ((1, 0), (0, 0)))
    return (first_half + second_half).reshape(-1)


def reference(adjoint, objective_gradient, diagonal, flux_blocks, flux_sensitivity, surface_mask, patch_band_slot, design_basis, condition_weights):
    def condition_solve(inputs):
        start_field, source, blocks, sensitivity = inputs

        def operate(values):
            return apply_operator(jnp.pad(values, ((0, 0), (1, 1), (1, 1), (1, 1))), diagonal, blocks)

        relaxed = start_field + (relaxation * (source - operate(start_field))) / diagonal
        smoothed = relaxed + (relaxation * (source - operate(relaxed))) / diagonal
        residual = source - operate(smoothed)
        surface = surface_mask.astype(jnp.float32) * jnp.sum(smoothed * sensitivity.astype(jnp.float32), axis=0)
        projected_gradient = jnp.dot(surface.reshape(-1, NZ), design_basis, precision=lax.Precision.HIGHEST, preferred_element_type=jnp.float32)
        slot_lookup = jax.ops.segment_sum(projected_gradient, patch_band_slot.reshape(-1), num_segments=BAND_SLOTS)
        return smoothed, residual, spread_bands(slot_lookup)

    smoothed, residual, gradients = lax.map(condition_solve, (adjoint, objective_gradient, flux_blocks, flux_sensitivity))
    weights_float = condition_weights.astype(jnp.float32)
    shares = weights_float / jnp.sum(weights_float)
    design_gradient = jnp.sum(shares[:, None] * gradients, axis=0)
    return smoothed, residual, design_gradient
```

```python
import functools

import jax
import jax.numpy as jnp
from jax import lax
from jax.experimental import pallas as pl
from jax.experimental.pallas import tpu as pltpu
from jax.sharding import PartitionSpec as P

NDES = 4096
RELAX = 0.8
LANES = 128
PAD = 8
MESH = pl.DeviceIdType.MESH


def spans_of(count):
    reach, out = 1, []
    while reach < count - 1:
        out.append(reach)
        reach *= 2
    return out


def kernel(
    sizes,
    adjoint,
    source_hbm,
    diagonal_hbm,
    flux_hbm,
    sensitivity_hbm,
    mask_hbm,
    slots_hbm,
    basis_hbm,
    weights_hbm,
    smoothed_out,
    residual_out,
    gradient_out,
    fields,
    source,
    diagonal,
    flux,
    sensitivity,
    mask,
    slots,
    basis,
    weights,
    surface,
    edges,
    row_halo,
    face_halo,
    step_edge,
    weight_edge,
    onehot,
    pieces,
    arrived,
    scalar_sems,
    local_sems,
    adjoint_sems,
    plane_sems,
    row_sems,
    face_sems,
    piece_sems,
    round_sems,
):
    n_cond, n_gx, n_yz = sizes
    devices = n_cond * n_gx * n_yz
    nvar, nx, ny, nz = source.shape
    halves = nz // LANES
    rows = pieces.shape[1]
    per_owner = NDES // (n_gx * n_yz)
    lines = NDES // LANES
    ci, xi, yi = lax.axis_index("cond"), lax.axis_index("gx"), lax.axis_index("yz")
    me = (ci * n_gx + xi) * n_yz + yi
    has_before_x, has_after_x = xi > 0, xi < n_gx - 1
    has_before_y, has_after_y = yi > 0, yi < n_yz - 1
    after_x, before_x = (ci, xi + 1, yi), (ci, xi - 1, yi)
    after_y, before_y = (ci, xi, yi + 1), (ci, xi, yi - 1)

    def signal(sem, target):
        pl.semaphore_signal(sem, inc=1, device_id=target, device_id_type=MESH)

    barrier = pltpu.get_barrier_semaphore()
    beside = n_cond - 1
    for there, target in (
        (has_before_x, before_x),
        (has_after_x, after_x),
        (has_before_y, before_y),
        (has_after_y, after_y),
    ):
        pl.when(there)(functools.partial(signal, barrier, target))
        beside = beside + there.astype(jnp.int32)
    for t in range(1, n_cond):
        signal(barrier, ((ci + t) % n_cond, xi, yi))

    spans = [slice(h * LANES, (h + 1) * LANES) for h in range(halves)]
    inner_y = pl.ds(PAD, ny)

    scalar_loads = [
        pltpu.make_async_copy(flux_hbm, flux, scalar_sems.at[0]),
        pltpu.make_async_copy(weights_hbm, weights, scalar_sems.at[1]),
    ]
    adjoint_loads = [
        pltpu.make_async_copy(
            adjoint.at[0, k, :, :, pl.ds(h * LANES, LANES)],
            fields.at[0, k, pl.ds(1, nx), h, inner_y, :],
            adjoint_sems.at[k, h],
        )
        for k in range(nvar)
        for h in range(halves)
    ]

    def plane_loads(x):
        return [
            pltpu.make_async_copy(source_hbm.at[0, :, x], source.at[:, x], plane_sems.at[0, x]),
            pltpu.make_async_copy(diagonal_hbm.at[x], diagonal.at[x], plane_sems.at[1, x]),
        ]

    late_loads = [
        pltpu.make_async_copy(src, dst, local_sems.at[i])
        for i, (src, dst) in enumerate(
            (
                (sensitivity_hbm.at[0], sensitivity),
                (mask_hbm, mask),
                (slots_hbm, slots),
                (basis_hbm, basis),
            )
        )
    ]
    for copy in adjoint_loads:
        copy.start()
    for copy in scalar_loads:
        copy.start()
    for x in range(nx):
        for copy in plane_loads(x):
            copy.start()
    for copy in late_loads:
        copy.start()

    blank = jnp.zeros((nvar, halves, ny, LANES), jnp.float32)
    blank_row = jnp.zeros((nvar, nx, halves, 1, LANES), jnp.float32)

    def outer(stage):
        return smoothed_out if stage == 2 else fields.at[stage]

    for stage in range(3):
        field = outer(stage)
        for x in (0, nx + 1):
            field[:, x, :, PAD : PAD + ny, :] = blank
        for y in (PAD - 1, PAD + ny):
            field[:, 1 : nx + 1, :, y : y + 1, :] = blank_row

    def clear_face(side):
        for stage in range(3):
            face_halo[stage, side] = blank

    def clear_row(side):
        for stage in range(3):
            row_halo[stage, side] = jnp.zeros((nvar, halves, nx, LANES), jnp.float32)

    pl.when(xi == 0)(functools.partial(clear_face, 0))
    pl.when(xi == n_gx - 1)(functools.partial(clear_face, 1))
    pl.when(yi == 0)(functools.partial(clear_row, 0))
    pl.when(yi == n_yz - 1)(functools.partial(clear_row, 1))

    def remote(src, dst, sems, target):
        return pltpu.make_async_remote_copy(
            src_ref=src,
            dst_ref=dst,
            send_sem=sems[0],
            recv_sem=sems[1],
            device_id=target,
            device_id_type=MESH,
        )

    def copies(stage):
        def face(x):
            return outer(stage).at[:, x, :, inner_y, :]

        def sems(ref, way):
            return ref.at[stage, 0, way], ref.at[stage, 1, way]

        up_x = remote(face(nx), face_halo.at[stage, 0], sems(face_sems, 0), after_x)
        down_x = remote(face(1), face_halo.at[stage, 1], sems(face_sems, 1), before_x)
        up_y = remote(edges.at[stage, 1], row_halo.at[stage, 0], sems(row_sems, 0), after_y)
        down_y = remote(edges.at[stage, 0], row_halo.at[stage, 1], sems(row_sems, 1), before_y)
        return (
            [(has_after_x, has_before_x, up_x), (has_before_x, has_after_x, down_x)],
            [(has_after_y, has_before_y, up_y), (has_before_y, has_after_y, down_y)],
        )

    def begin(plans):
        for go, _, copy in plans:
            pl.when(go)(copy.start)

    def receive(plans):
        for _, come, copy in plans:
            pl.when(come)(copy.wait_recv)

    def drain(plans):
        for go, _, copy in plans:
            pl.when(go)(copy.wait_send)

    def line_round(distances):
        targets = []
        for axis, distance in distances:
            here, count = (xi, n_gx) if axis == "gx" else (yi, n_yz)
            for sign in (1, -1):
                there = here + sign * distance
                target = (ci, there, yi) if axis == "gx" else (ci, xi, there)
                targets.append((jnp.logical_and(there >= 0, there < count), target))
        return targets

    gx_spans, yz_spans = spans_of(n_gx), spans_of(n_yz)
    rounds = []
    for i in range(max(len(gx_spans), len(yz_spans))):
        distances = [("gx", d) for d in gx_spans[i : i + 1]] + [("yz", d) for d in yz_spans[i : i + 1]]
        rounds.append(line_round(distances))
    always = ci >= 0
    rounds.append([(always, (ci, (xi + t) % n_gx, yi)) for t in range(1, n_gx)])
    rounds.append([(always, ((ci + t) % n_cond, xi, yi)) for t in range(1, n_cond)])

    def tell(i):
        for there, target in rounds[i]:
            pl.when(there)(functools.partial(signal, round_sems.at[i], target))

    def hear(i):
        count = 0
        for there, _ in rounds[i]:
            count = count + there.astype(jnp.int32)
        pl.semaphore_wait(round_sems.at[i], count)

    def advance(i):
        hear(i)
        if i + 1 < len(rounds):
            tell(i + 1)

    for copy in adjoint_loads:
        copy.wait()
    for x in range(nx):
        for k in range(nvar):
            for h in range(halves):
                edges[0, 0, k, h, x : x + 1, :] = fields[0, k, x + 1, h, PAD : PAD + 1, :]
                last = PAD + ny - 1
                edges[0, 1, k, h, x : x + 1, :] = fields[0, k, x + 1, h, last : last + 1, :]
    pl.semaphore_wait(barrier, beside)
    for plans in copies(0):
        begin(plans)
    tell(0)
    for copy in scalar_loads:
        copy.wait()

    lane = lax.broadcasted_iota(jnp.int32, (ny, LANES), 1)

    def gathered(stage, x):
        field = outer(stage)
        acc = [[source[k, x, :, s] for s in spans] for k in range(nvar)]
        centres = []
        for e in range(nvar):
            centre = [field[e, x + 1, h, PAD : PAD + ny, :] for h in range(halves)]
            centres.append(centre)
            up = [pltpu.roll(c, LANES - 1, 1) for c in centre] + [jnp.zeros((ny, LANES), jnp.float32)]
            down = [jnp.zeros((ny, LANES), jnp.float32)] + [pltpu.roll(c, 1, 1) for c in centre]
            shifted = (
                [field[e, x + 2, h, PAD : PAD + ny, :] for h in range(halves)],
                [field[e, x, h, PAD : PAD + ny, :] for h in range(halves)],
                [field[e, x + 1, h, PAD + 1 : PAD + ny + 1, :] for h in range(halves)],
                [field[e, x + 1, h, PAD - 1 : PAD + ny - 1, :] for h in range(halves)],
                [jnp.where(lane == LANES - 1, up[h + 1], up[h]) for h in range(halves)],
                [jnp.where(lane == 0, down[h], down[h + 1]) for h in range(halves)],
            )
            for d in range(6):
                for k in range(nvar):
                    scale = flux[e, k, 0, d]
                    for h in range(halves):
                        acc[k][h] = acc[k][h] + scale * shifted[d][h]
        return acc, centres

    def keep_edges(stage, k, h, x, value):
        edges[stage, 0, k, h, pl.ds(x, 1), :] = value[0:1]
        edges[stage, 1, k, h, pl.ds(x, 1), :] = value[ny - 1 : ny]

    def relax(stage, x, carry):
        if stage == 0:
            for copy in plane_loads(x):
                copy.wait()
        acc, centres = gathered(stage, x)
        step = [RELAX / diagonal[x, :, s] for s in spans]
        total = [None] * halves
        for h in range(halves):
            if stage == 0:
                step_edge[0, h, pl.ds(x, 1), :] = step[h][0:1]
                step_edge[1, h, pl.ds(x, 1), :] = step[h][ny - 1 : ny]
            else:
                cover = mask[x, :, spans[h]].astype(jnp.float32)
            for k in range(nvar):
                value = (1.0 - RELAX) * centres[k][h] + step[h] * acc[k][h]
                outer(stage + 1)[k, x + 1, h, PAD : PAD + ny, :] = value
                keep_edges(stage + 1, k, h, x, value)
                if stage == 1:
                    weight = sensitivity[k, x, :, spans[h]].astype(jnp.float32) * cover
                    weight_edge[0, k, h, pl.ds(x, 1), :] = weight[0:1]
                    weight_edge[1, k, h, pl.ds(x, 1), :] = weight[ny - 1 : ny]
                    term = value * weight
                    total[h] = term if k == 0 else total[h] + term
            if stage == 1:
                surface[x, :, spans[h]] = total[h]
        return carry

    def settle(x, carry):
        acc, centres = gathered(2, x)
        for k in range(nvar):
            for h in range(halves):
                value = acc[k][h] - diagonal[x, :, spans[h]] * centres[k][h]
                residual_out[0, k, x, :, spans[h]] = value
                keep_edges(3, k, h, x, value)
        return carry

    def brought(halo, h, d):
        cells = [halo[e, h] for e in range(nvar)]
        out = []
        for k in range(nvar):
            total = flux[0, k, 0, d] * cells[0]
            for e in range(1, nvar):
                total = total + flux[e, k, 0, d] * cells[e]
            out.append(total)
        return out

    def add_faces(stage):
        for side, x, d in ((0, 0, 1), (1, nx - 1, 0)):
            for h in range(halves):
                more = brought(face_halo.at[stage, side], h, d)
                if stage < 2:
                    step = RELAX / diagonal[x, :, spans[h]]
                total = None
                for k in range(nvar):
                    if stage == 2:
                        value = residual_out[0, k, x, :, spans[h]] + more[k]
                        residual_out[0, k, x, :, spans[h]] = value
                    else:
                        part = step * more[k]
                        value = outer(stage + 1)[k, x + 1, h, PAD : PAD + ny, :] + part
                        outer(stage + 1)[k, x + 1, h, PAD : PAD + ny, :] = value
                        if stage == 1:
                            term = part * sensitivity[k, x, :, spans[h]].astype(jnp.float32)
                            total = term if k == 0 else total + term
                    keep_edges(stage + 1, k, h, x, value)
                if stage == 1:
                    cover = mask[x, :, spans[h]].astype(jnp.float32)
                    surface[x, :, spans[h]] = surface[x, :, spans[h]] + total * cover

    def add_rows(stage):
        for side, y, d in ((0, 0, 3), (1, ny - 1, 2)):
            for h in range(halves):
                more = brought(row_halo.at[stage, side], h, d)
                total = None
                for k in range(nvar):
                    part = more[k] if stage == 2 else step_edge[side, h] * more[k]
                    value = edges[stage + 1, side, k, h] + part
                    if stage < 2:
                        edges[stage + 1, side, k, h] = value
                    if stage == 1:
                        term = part * weight_edge[side, k, h]
                        total = term if k == 0 else total + term
                    for x in range(nx):
                        if stage == 2:
                            residual_out[0, k, x, y : y + 1, spans[h]] = value[x : x + 1]
                        else:
                            outer(stage + 1)[k, x + 1, h, PAD + y : PAD + y + 1, :] = value[x : x + 1]
                if stage == 1:
                    for x in range(nx):
                        line = surface[x, y : y + 1, spans[h]]
                        surface[x, y : y + 1, spans[h]] = line + total[x : x + 1]

    def complete(stage):
        faces, ranks = copies(stage)
        receive(faces)
        add_faces(stage)
        receive(ranks)
        add_rows(stage)

    lax.fori_loop(0, nx, functools.partial(relax, 0), 0)
    advance(0)
    complete(0)
    for plans in copies(1):
        begin(plans)
    for i in range(1, len(rounds) - 2):
        advance(i)

    for copy in late_loads:
        copy.wait()

    def relax_and_advance(x, carry):
        relax(1, x, carry)

        @pl.when(x == nx // 2)
        def _():
            advance(len(rounds) - 2)

        return carry

    lax.fori_loop(0, nx, relax_and_advance, 0)

    def split(value):
        high = value.astype(jnp.bfloat16)
        return high, (value - high.astype(jnp.float32)).astype(jnp.bfloat16)

    line = lax.broadcasted_iota(jnp.int32, (lines, nx * ny), 0)
    spots = jnp.concatenate([slots[x : x + 1, :] for x in range(nx)], axis=1)
    wanted = jnp.concatenate([2 * line, 2 * line + 1, 2 * line - 1], axis=0)
    onehot[...] = (wanted == spots).astype(jnp.float32).astype(jnp.bfloat16)
    weight_sum = weights[0]
    for c in range(1, n_cond):
        weight_sum = weight_sum + weights[c]
    share = jnp.full((1, LANES), weights[ci], jnp.int32).astype(jnp.float32) / jnp.full(
        (1, LANES), weight_sum, jnp.int32
    ).astype(jnp.float32)

    complete(1)
    for plans in copies(2):
        begin(plans)

    dot = functools.partial(jnp.dot, preferred_element_type=jnp.float32)
    basis_high, basis_low = split(basis[...])
    surface_high, surface_low = split(surface[...].reshape(nx * ny, nz))
    projected = (
        dot(surface_high, basis_high) + dot(surface_high, basis_low) + dot(surface_low, basis_high)
    )
    high, low = split(projected)
    looked = dot(onehot[...], high) + dot(onehot[...], low)
    turned = pltpu.roll(looked[lines:], LANES // 2, 1)
    column = lax.broadcasted_iota(jnp.int32, (lines, LANES), 1)
    gradient = looked[:lines] + jnp.where(column < LANES // 2, turned[lines:], turned[:lines])
    gradient = gradient * share
    for g in range(lines // rows):
        pieces[g] = gradient[g * rows : (g + 1) * rows]

    def group(gx, yz):
        return (gx * n_yz + yz) * per_owner // (rows * LANES)

    def give(c, gx, yz):
        remote(
            pieces.at[group(gx, yz)],
            arrived.at[me],
            (piece_sems.at[0], piece_sems.at[1]),
            (c, gx, yz),
        ).start()

    arrived[me] = pieces[group(xi, yi)]
    advance(len(rounds) - 1)
    if devices <= 64:
        for dy in range(n_yz):
            for dx in range(n_gx):
                for dc in range(n_cond):
                    if dc or dx or dy:
                        give((ci + dc) % n_cond, (xi + dx) % n_gx, (yi + dy) % n_yz)
    else:

        def give_next(t, carry):
            flat = (me + t) % devices
            give(flat // (n_gx * n_yz), (flat // n_yz) % n_gx, flat % n_yz)
            return carry

        lax.fori_loop(1, devices, give_next, 0)

    lax.fori_loop(0, nx, settle, 0)
    others = arrived.at[pl.ds(0, devices - 1)]
    for i in range(2):
        pltpu.make_async_copy(others, others, piece_sems.at[i]).wait()
    gradient_out[...] = jnp.sum(arrived[...], axis=0)
    complete(2)
    for stage in range(3):
        for plans in copies(stage):
            drain(plans)


def write(padded, residual, gradient, smoothed_hbm, residual_hbm, gradient_hbm, sems):
    nvar, planes, halves = padded.shape[:3]
    nx, ny = planes - 2, smoothed_hbm.shape[3]
    stores = [
        pltpu.make_async_copy(
            padded.at[:, pl.ds(1, nx), h, pl.ds(PAD, ny), :],
            smoothed_hbm.at[0, :, :, :, pl.ds(h * LANES, LANES)],
            sems.at[2 + h],
        )
        for h in range(halves)
    ]
    stores.append(pltpu.make_async_copy(residual, residual_hbm, sems.at[0]))
    stores.append(pltpu.make_async_copy(gradient, gradient_hbm, sems.at[1]))
    for copy in stores:
        copy.start()
    for copy in stores:
        copy.wait()


def local(
    adjoint,
    objective_gradient,
    diagonal,
    flux_blocks,
    flux_sensitivity,
    surface_mask,
    patch_band_slot,
    design_basis,
    condition_weights,
):
    sizes = tuple(lax.axis_size(axis) for axis in ("cond", "gx", "yz"))
    devices = sizes[0] * sizes[1] * sizes[2]
    _, nvar, nx, ny, nz = adjoint.shape
    halves = nz // LANES
    per_owner = NDES // (sizes[1] * sizes[2])
    rows = max(1, per_owner // LANES)
    lines = NDES // LANES
    rounds = max(len(spans_of(sizes[1])), len(spans_of(sizes[2]))) + 2
    f32 = jnp.float32
    hbm = pl.BlockSpec(memory_space=pltpu.MemorySpace.HBM)
    vmem = pl.BlockSpec(memory_space=pltpu.MemorySpace.VMEM)
    padded = (nvar, nx + 2, halves, ny + 2 * PAD, LANES)
    grant = 67043328 - 2**16 - 4 * (adjoint.size + 2 * adjoint.size * (nx + 2) * (ny + 2 * PAD) // (nx * ny))
    smoothed, residual, gradient = pl.pallas_call(
        functools.partial(kernel, sizes),
        out_shape=(
            pltpu.VMEM(padded, f32),
            pltpu.VMEM(adjoint.shape, f32),
            pltpu.VMEM((rows, LANES), f32),
        ),
        in_specs=[hbm] * 9,
        out_specs=(vmem, vmem, vmem),
        scratch_shapes=[
            pltpu.VMEM((2,) + padded, f32),
            pltpu.VMEM((nvar, nx, ny, nz), f32),
            pltpu.VMEM((nx, ny, nz), f32),
            pltpu.SMEM((nvar, nvar, 1, 6), f32),
            pltpu.VMEM((nvar, nx, ny, nz), jnp.bfloat16),
            pltpu.VMEM((nx, ny, nz), jnp.int32),
            pltpu.VMEM((nx, ny), jnp.int32),
            pltpu.VMEM(design_basis.shape, f32),
            pltpu.SMEM(condition_weights.shape, jnp.int32),
            pltpu.VMEM((nx, ny, nz), f32),
            pltpu.VMEM((4, 2, nvar, halves, nx, LANES), f32),
            pltpu.VMEM((3, 2, nvar, halves, nx, LANES), f32),
            pltpu.VMEM((3, 2, nvar, halves, ny, LANES), f32),
            pltpu.VMEM((2, halves, nx, LANES), f32),
            pltpu.VMEM((2, nvar, halves, nx, LANES), f32),
            pltpu.VMEM((3 * lines, nx * ny), jnp.bfloat16),
            pltpu.VMEM((NDES // (rows * LANES), rows, LANES), f32),
            pltpu.VMEM((devices, rows, LANES), f32),
            pltpu.SemaphoreType.DMA((2,)),
            pltpu.SemaphoreType.DMA((4,)),
            pltpu.SemaphoreType.DMA((nvar, halves)),
            pltpu.SemaphoreType.DMA((2, nx)),
            pltpu.SemaphoreType.DMA((3, 2, 2)),
            pltpu.SemaphoreType.DMA((3, 2, 2)),
            pltpu.SemaphoreType.DMA((2,)),
            pltpu.SemaphoreType.REGULAR((rounds,)),
        ],
        compiler_params=pltpu.CompilerParams(
            collective_id=0, has_side_effects=True, vmem_limit_bytes=grant
        ),
    )(
        adjoint,
        objective_gradient,
        diagonal,
        jnp.transpose(flux_blocks, (2, 3, 0, 1)),
        flux_sensitivity,
        surface_mask,
        patch_band_slot,
        design_basis,
        condition_weights,
    )
    smoothed, residual, gradient = pl.pallas_call(
        write,
        out_shape=(
            jax.ShapeDtypeStruct(adjoint.shape, f32),
            jax.ShapeDtypeStruct(adjoint.shape, f32),
            jax.ShapeDtypeStruct((rows, LANES), f32),
        ),
        in_specs=[vmem] * 3,
        out_specs=(hbm, hbm, hbm),
        scratch_shapes=[pltpu.SemaphoreType.DMA((2 + halves,))],
    )(smoothed, residual, gradient)
    flat = gradient.reshape(-1)
    if per_owner < flat.shape[0]:
        owner = lax.axis_index(("gx", "yz"))
        flat = lax.dynamic_slice_in_dim(flat, (owner * per_owner) % flat.shape[0], per_owner, 0)
    return smoothed, residual, flat


def solution(mesh):
    placed = (
        P("cond", None, "gx", "yz", None),
        P("cond", None, "gx", "yz", None),
        P("gx", "yz", None),
        P("cond", None, None, None),
        P("cond", None, "gx", "yz", None),
        P("gx", "yz", None),
        P("gx", "yz"),
        P(),
        P(),
    )
    return jax.shard_map(
        local,
        mesh=mesh,
        in_specs=placed,
        out_specs=(
            P("cond", None, "gx", "yz", None),
            P("cond", None, "gx", "yz", None),
            P(("gx", "yz")),
        ),
        check_vma=False,
    )
```

```python
import functools

import jax
import jax.numpy as jnp
from jax import lax
from jax.experimental import pallas as pl
from jax.experimental.pallas import tpu as pltpu
from jax.sharding import PartitionSpec as P

NDES = 4096
RELAX = 0.8
LANES = 128
PAD = 8
MESH = pl.DeviceIdType.MESH


def spans_of(count):
    reach, out = 1, []
    while reach < count - 1:
        out.append(reach)
        reach *= 2
    return out


def kernel(
    sizes,
    adjoint,
    source_hbm,
    diagonal_hbm,
    flux_hbm,
    sensitivity_hbm,
    mask_hbm,
    slots_hbm,
    basis_hbm,
    weights_hbm,
    smoothed_out,
    residual_out,
    gradient_out,
    fields,
    source,
    diagonal,
    flux,
    sensitivity,
    mask,
    slots,
    basis,
    weights,
    surface,
    edges,
    row_halo,
    face_halo,
    step_edge,
    weight_edge,
    onehot,
    pieces,
    arrived,
    scalar_sems,
    local_sems,
    adjoint_sems,
    plane_sems,
    row_sems,
    face_sems,
    piece_sems,
    round_sems,
):
    n_cond, n_gx, n_yz = sizes
    devices = n_cond * n_gx * n_yz
    nvar, nx, ny, nz = source.shape
    halves = nz // LANES
    rows = pieces.shape[1]
    per_owner = NDES // (n_gx * n_yz)
    lines = NDES // LANES
    ci, xi, yi = lax.axis_index("cond"), lax.axis_index("gx"), lax.axis_index("yz")
    me = (ci * n_gx + xi) * n_yz + yi
    has_before_x, has_after_x = xi > 0, xi < n_gx - 1
    has_before_y, has_after_y = yi > 0, yi < n_yz - 1
    after_x, before_x = (ci, xi + 1, yi), (ci, xi - 1, yi)
    after_y, before_y = (ci, xi, yi + 1), (ci, xi, yi - 1)

    def signal(sem, target):
        pl.semaphore_signal(sem, inc=1, device_id=target, device_id_type=MESH)

    barrier = pltpu.get_barrier_semaphore()
    beside = n_cond - 1
    for there, target in (
        (has_before_x, before_x),
        (has_after_x, after_x),
        (has_before_y, before_y),
        (has_after_y, after_y),
    ):
        pl.when(there)(functools.partial(signal, barrier, target))
        beside = beside + there.astype(jnp.int32)
    for t in range(1, n_cond):
        signal(barrier, ((ci + t) % n_cond, xi, yi))

    spans = [slice(h * LANES, (h + 1) * LANES) for h in range(halves)]
    inner_y = pl.ds(PAD, ny)

    scalar_loads = [
        pltpu.make_async_copy(flux_hbm, flux, scalar_sems.at[0]),
        pltpu.make_async_copy(weights_hbm, weights, scalar_sems.at[1]),
    ]
    adjoint_loads = [
        pltpu.make_async_copy(
            adjoint.at[0, k, :, :, pl.ds(h * LANES, LANES)],
            fields.at[0, k, pl.ds(1, nx), h, inner_y, :],
            adjoint_sems.at[k, h],
        )
        for k in range(nvar)
        for h in range(halves)
    ]

    def plane_loads(x):
        return [
            pltpu.make_async_copy(source_hbm.at[0, :, x], source.at[:, x], plane_sems.at[0, x]),
            pltpu.make_async_copy(diagonal_hbm.at[x], diagonal.at[x], plane_sems.at[1, x]),
        ]

    late_loads = [
        pltpu.make_async_copy(src, dst, local_sems.at[i])
        for i, (src, dst) in enumerate(
            (
                (sensitivity_hbm.at[0], sensitivity),
                (mask_hbm, mask),
                (slots_hbm, slots),
                (basis_hbm, basis),
            )
        )
    ]
    for copy in adjoint_loads:
        copy.start()
    for copy in scalar_loads:
        copy.start()
    for x in range(nx):
        for copy in plane_loads(x):
            copy.start()
    for copy in late_loads:
        copy.start()

    blank = jnp.zeros((nvar, halves, ny, LANES), jnp.float32)
    blank_row = jnp.zeros((nvar, nx, halves, 1, LANES), jnp.float32)

    def outer(stage):
        return smoothed_out if stage == 2 else fields.at[stage]

    for stage in range(3):
        field = outer(stage)
        for x in (0, nx + 1):
            field[:, x, :, PAD : PAD + ny, :] = blank
        for y in (PAD - 1, PAD + ny):
            field[:, 1 : nx + 1, :, y : y + 1, :] = blank_row

    def clear_face(side):
        for stage in range(3):
            face_halo[stage, side] = blank

    def clear_row(side):
        for stage in range(3):
            row_halo[stage, side] = jnp.zeros((nvar, halves, nx, LANES), jnp.float32)

    pl.when(xi == 0)(functools.partial(clear_face, 0))
    pl.when(xi == n_gx - 1)(functools.partial(clear_face, 1))
    pl.when(yi == 0)(functools.partial(clear_row, 0))
    pl.when(yi == n_yz - 1)(functools.partial(clear_row, 1))

    def remote(src, dst, sems, target):
        return pltpu.make_async_remote_copy(
            src_ref=src,
            dst_ref=dst,
            send_sem=sems[0],
            recv_sem=sems[1],
            device_id=target,
            device_id_type=MESH,
        )

    def copies(stage):
        def face(x):
            return outer(stage).at[:, x, :, inner_y, :]

        def sems(ref, way):
            return ref.at[stage, 0, way], ref.at[stage, 1, way]

        up_x = remote(face(nx), face_halo.at[stage, 0], sems(face_sems, 0), after_x)
        down_x = remote(face(1), face_halo.at[stage, 1], sems(face_sems, 1), before_x)
        up_y = remote(edges.at[stage, 1], row_halo.at[stage, 0], sems(row_sems, 0), after_y)
        down_y = remote(edges.at[stage, 0], row_halo.at[stage, 1], sems(row_sems, 1), before_y)
        return (
            [(has_after_x, has_before_x, up_x), (has_before_x, has_after_x, down_x)],
            [(has_after_y, has_before_y, up_y), (has_before_y, has_after_y, down_y)],
        )

    def begin(plans):
        for go, _, copy in plans:
            pl.when(go)(copy.start)

    def receive(plans):
        for _, come, copy in plans:
            pl.when(come)(copy.wait_recv)

    def drain(plans):
        for go, _, copy in plans:
            pl.when(go)(copy.wait_send)

    def line_round(distances):
        targets = []
        for axis, distance in distances:
            here, count = (xi, n_gx) if axis == "gx" else (yi, n_yz)
            for sign in (1, -1):
                there = here + sign * distance
                target = (ci, there, yi) if axis == "gx" else (ci, xi, there)
                targets.append((jnp.logical_and(there >= 0, there < count), target))
        return targets

    gx_spans, yz_spans = spans_of(n_gx), spans_of(n_yz)
    rounds = []
    for i in range(max(len(gx_spans), len(yz_spans))):
        distances = [("gx", d) for d in gx_spans[i : i + 1]] + [("yz", d) for d in yz_spans[i : i + 1]]
        rounds.append(line_round(distances))
    always = ci >= 0
    rounds.append([(always, (ci, (xi + t) % n_gx, yi)) for t in range(1, n_gx)])
    rounds.append([(always, ((ci + t) % n_cond, xi, yi)) for t in range(1, n_cond)])

    def tell(i):
        for there, target in rounds[i]:
            pl.when(there)(functools.partial(signal, round_sems.at[i], target))

    def hear(i):
        count = 0
        for there, _ in rounds[i]:
            count = count + there.astype(jnp.int32)
        pl.semaphore_wait(round_sems.at[i], count)

    def advance(i):
        hear(i)
        if i + 1 < len(rounds):
            tell(i + 1)

    for copy in adjoint_loads:
        copy.wait()
    for x in range(nx):
        for k in range(nvar):
            for h in range(halves):
                edges[0, 0, k, h, x : x + 1, :] = fields[0, k, x + 1, h, PAD : PAD + 1, :]
                last = PAD + ny - 1
                edges[0, 1, k, h, x : x + 1, :] = fields[0, k, x + 1, h, last : last + 1, :]
    pl.semaphore_wait(barrier, beside)
    for plans in copies(0):
        begin(plans)
    tell(0)
    for copy in scalar_loads:
        copy.wait()

    lane = lax.broadcasted_iota(jnp.int32, (ny, LANES), 1)

    def gathered(stage, x):
        field = outer(stage)
        acc = [[source[k, x, :, s] for s in spans] for k in range(nvar)]
        centres = []
        for e in range(nvar):
            centre = [field[e, x + 1, h, PAD : PAD + ny, :] for h in range(halves)]
            centres.append(centre)
            up = [pltpu.roll(c, LANES - 1, 1) for c in centre] + [jnp.zeros((ny, LANES), jnp.float32)]
            down = [jnp.zeros((ny, LANES), jnp.float32)] + [pltpu.roll(c, 1, 1) for c in centre]
            shifted = (
                [field[e, x + 2, h, PAD : PAD + ny, :] for h in range(halves)],
                [field[e, x, h, PAD : PAD + ny, :] for h in range(halves)],
                [field[e, x + 1, h, PAD + 1 : PAD + ny + 1, :] for h in range(halves)],
                [field[e, x + 1, h, PAD - 1 : PAD + ny - 1, :] for h in range(halves)],
                [jnp.where(lane == LANES - 1, up[h + 1], up[h]) for h in range(halves)],
                [jnp.where(lane == 0, down[h], down[h + 1]) for h in range(halves)],
            )
            for d in range(6):
                for k in range(nvar):
                    scale = flux[e, k, 0, d]
                    for h in range(halves):
                        acc[k][h] = acc[k][h] + scale * shifted[d][h]
        return acc, centres

    def keep_edges(stage, k, h, x, value):
        edges[stage, 0, k, h, pl.ds(x, 1), :] = value[0:1]
        edges[stage, 1, k, h, pl.ds(x, 1), :] = value[ny - 1 : ny]

    def relax(stage, x, carry):
        if stage == 0:
            for copy in plane_loads(x):
                copy.wait()
        acc, centres = gathered(stage, x)
        step = [RELAX / diagonal[x, :, s] for s in spans]
        total = [None] * halves
        for h in range(halves):
            if stage == 0:
                step_edge[0, h, pl.ds(x, 1), :] = step[h][0:1]
                step_edge[1, h, pl.ds(x, 1), :] = step[h][ny - 1 : ny]
            else:
                cover = mask[x, :, spans[h]].astype(jnp.float32)
            for k in range(nvar):
                value = (1.0 - RELAX) * centres[k][h] + step[h] * acc[k][h]
                outer(stage + 1)[k, x + 1, h, PAD : PAD + ny, :] = value
                keep_edges(stage + 1, k, h, x, value)
                if stage == 1:
                    weight = sensitivity[k, x, :, spans[h]].astype(jnp.float32) * cover
                    weight_edge[0, k, h, pl.ds(x, 1), :] = weight[0:1]
                    weight_edge[1, k, h, pl.ds(x, 1), :] = weight[ny - 1 : ny]
                    term = value * weight
                    total[h] = term if k == 0 else total[h] + term
            if stage == 1:
                surface[x, :, spans[h]] = total[h]
        return carry

    def settle(x, carry):
        acc, centres = gathered(2, x)
        for k in range(nvar):
            for h in range(halves):
                value = acc[k][h] - diagonal[x, :, spans[h]] * centres[k][h]
                residual_out[0, k, x, :, spans[h]] = value
                keep_edges(3, k, h, x, value)
        return carry

    def brought(halo, h, d):
        cells = [halo[e, h] for e in range(nvar)]
        out = []
        for k in range(nvar):
            total = flux[0, k, 0, d] * cells[0]
            for e in range(1, nvar):
                total = total + flux[e, k, 0, d] * cells[e]
            out.append(total)
        return out

    def add_faces(stage):
        for side, x, d in ((0, 0, 1), (1, nx - 1, 0)):
            for h in range(halves):
                more = brought(face_halo.at[stage, side], h, d)
                if stage < 2:
                    step = RELAX / diagonal[x, :, spans[h]]
                total = None
                for k in range(nvar):
                    if stage == 2:
                        value = residual_out[0, k, x, :, spans[h]] + more[k]
                        residual_out[0, k, x, :, spans[h]] = value
                    else:
                        part = step * more[k]
                        value = outer(stage + 1)[k, x + 1, h, PAD : PAD + ny, :] + part
                        outer(stage + 1)[k, x + 1, h, PAD : PAD + ny, :] = value
                        if stage == 1:
                            term = part * sensitivity[k, x, :, spans[h]].astype(jnp.float32)
                            total = term if k == 0 else total + term
                    keep_edges(stage + 1, k, h, x, value)
                if stage == 1:
                    cover = mask[x, :, spans[h]].astype(jnp.float32)
                    surface[x, :, spans[h]] = surface[x, :, spans[h]] + total * cover

    def add_rows(stage):
        for side, y, d in ((0, 0, 3), (1, ny - 1, 2)):
            for h in range(halves):
                more = brought(row_halo.at[stage, side], h, d)
                total = None
                for k in range(nvar):
                    part = more[k] if stage == 2 else step_edge[side, h] * more[k]
                    value = edges[stage + 1, side, k, h] + part
                    if stage < 2:
                        edges[stage + 1, side, k, h] = value
                    if stage == 1:
                        term = part * weight_edge[side, k, h]
                        total = term if k == 0 else total + term
                    for x in range(nx):
                        if stage == 2:
                            residual_out[0, k, x, y : y + 1, spans[h]] = value[x : x + 1]
                        else:
                            outer(stage + 1)[k, x + 1, h, PAD + y : PAD + y + 1, :] = value[x : x + 1]
                if stage == 1:
                    for x in range(nx):
                        line = surface[x, y : y + 1, spans[h]]
                        surface[x, y : y + 1, spans[h]] = line + total[x : x + 1]

    def complete(stage):
        faces, ranks = copies(stage)
        receive(faces)
        add_faces(stage)
        receive(ranks)
        add_rows(stage)

    lax.fori_loop(0, nx, functools.partial(relax, 0), 0)
    advance(0)
    complete(0)
    for plans in copies(1):
        begin(plans)
    for i in range(1, len(rounds) - 2):
        advance(i)

    for copy in late_loads:
        copy.wait()

    def relax_and_advance(x, carry):
        relax(1, x, carry)

        @pl.when(x == nx // 2)
        def _():
            advance(len(rounds) - 2)

        return carry

    lax.fori_loop(0, nx, relax_and_advance, 0)

    def split(value):
        high = value.astype(jnp.bfloat16)
        return high, (value - high.astype(jnp.float32)).astype(jnp.bfloat16)

    line = lax.broadcasted_iota(jnp.int32, (lines, nx * ny), 0)
    spots = jnp.concatenate([slots[x : x + 1, :] for x in range(nx)], axis=1)
    wanted = jnp.concatenate([2 * line, 2 * line + 1, 2 * line - 1], axis=0)
    onehot[...] = (wanted == spots).astype(jnp.float32).astype(jnp.bfloat16)
    weight_sum = weights[0]
    for c in range(1, n_cond):
        weight_sum = weight_sum + weights[c]
    share = jnp.full((1, LANES), weights[ci], jnp.int32).astype(jnp.float32) / jnp.full(
        (1, LANES), weight_sum, jnp.int32
    ).astype(jnp.float32)

    complete(1)
    for plans in copies(2):
        begin(plans)

    dot = functools.partial(jnp.dot, preferred_element_type=jnp.float32)
    basis_high, basis_low = split(basis[...])
    surface_high, surface_low = split(surface[...].reshape(nx * ny, nz))
    projected = (
        dot(surface_high, basis_high) + dot(surface_high, basis_low) + dot(surface_low, basis_high)
    )
    high, low = split(projected)
    looked = dot(onehot[...], high) + dot(onehot[...], low)
    turned = pltpu.roll(looked[lines:], LANES // 2, 1)
    column = lax.broadcasted_iota(jnp.int32, (lines, LANES), 1)
    gradient = looked[:lines] + jnp.where(column < LANES // 2, turned[lines:], turned[:lines])
    gradient = gradient * share
    for g in range(lines // rows):
        pieces[g] = gradient[g * rows : (g + 1) * rows]

    def group(gx, yz):
        return (gx * n_yz + yz) * per_owner // (rows * LANES)

    def give(c, gx, yz):
        remote(
            pieces.at[group(gx, yz)],
            arrived.at[me],
            (piece_sems.at[0], piece_sems.at[1]),
            (c, gx, yz),
        ).start()

    arrived[me] = pieces[group(xi, yi)]
    advance(len(rounds) - 1)
    if devices <= 64:
        for dy in range(n_yz):
            for dx in range(n_gx):
                for dc in range(n_cond):
                    if dc or dx or dy:
                        give((ci + dc) % n_cond, (xi + dx) % n_gx, (yi + dy) % n_yz)
    else:

        def give_next(t, carry):
            flat = (me + t) % devices
            give(flat // (n_gx * n_yz), (flat // n_yz) % n_gx, flat % n_yz)
            return carry

        lax.fori_loop(1, devices, give_next, 0)

    lax.fori_loop(0, nx, settle, 0)
    others = arrived.at[pl.ds(0, devices - 1)]
    for i in range(2):
        pltpu.make_async_copy(others, others, piece_sems.at[i]).wait()
    gradient_out[...] = jnp.sum(arrived[...], axis=0)
    complete(2)
    for stage in range(3):
        for plans in copies(stage):
            drain(plans)


def write(padded, residual, gradient, smoothed_hbm, residual_hbm, gradient_hbm, sems):
    nvar, planes, halves = padded.shape[:3]
    nx, ny = planes - 2, smoothed_hbm.shape[3]
    stores = [
        pltpu.make_async_copy(
            padded.at[:, pl.ds(1, nx), h, pl.ds(PAD, ny), :],
            smoothed_hbm.at[0, :, :, :, pl.ds(h * LANES, LANES)],
            sems.at[2 + h],
        )
        for h in range(halves)
    ]
    stores.append(pltpu.make_async_copy(residual, residual_hbm, sems.at[0]))
    stores.append(pltpu.make_async_copy(gradient, gradient_hbm, sems.at[1]))
    for copy in stores:
        copy.start()
    for copy in stores:
        copy.wait()


def local(
    adjoint,
    objective_gradient,
    diagonal,
    flux_blocks,
    flux_sensitivity,
    surface_mask,
    patch_band_slot,
    design_basis,
    condition_weights,
):
    sizes = tuple(lax.axis_size(axis) for axis in ("cond", "gx", "yz"))
    devices = sizes[0] * sizes[1] * sizes[2]
    _, nvar, nx, ny, nz = adjoint.shape
    halves = nz // LANES
    per_owner = NDES // (sizes[1] * sizes[2])
    rows = max(1, per_owner // LANES)
    lines = NDES // LANES
    rounds = max(len(spans_of(sizes[1])), len(spans_of(sizes[2]))) + 2
    f32 = jnp.float32
    hbm = pl.BlockSpec(memory_space=pltpu.MemorySpace.HBM)
    vmem = pl.BlockSpec(memory_space=pltpu.MemorySpace.VMEM)
    padded = (nvar, nx + 2, halves, ny + 2 * PAD, LANES)
    grant = 67043328 - 2**16 - 4 * (adjoint.size + 2 * adjoint.size * (nx + 2) * (ny + 2 * PAD) // (nx * ny))
    smoothed, residual, gradient = pl.pallas_call(
        functools.partial(kernel, sizes),
        out_shape=(
            pltpu.VMEM(padded, f32),
            pltpu.VMEM(adjoint.shape, f32),
            pltpu.VMEM((rows, LANES), f32),
        ),
        in_specs=[hbm] * 9,
        out_specs=(vmem, vmem, vmem),
        scratch_shapes=[
            pltpu.VMEM((2,) + padded, f32),
            pltpu.VMEM((nvar, nx, ny, nz), f32),
            pltpu.VMEM((nx, ny, nz), f32),
            pltpu.SMEM((nvar, nvar, 1, 6), f32),
            pltpu.VMEM((nvar, nx, ny, nz), jnp.bfloat16),
            pltpu.VMEM((nx, ny, nz), jnp.int32),
            pltpu.VMEM((nx, ny), jnp.int32),
            pltpu.VMEM(design_basis.shape, f32),
            pltpu.SMEM(condition_weights.shape, jnp.int32),
            pltpu.VMEM((nx, ny, nz), f32),
            pltpu.VMEM((4, 2, nvar, halves, nx, LANES), f32),
            pltpu.VMEM((3, 2, nvar, halves, nx, LANES), f32),
            pltpu.VMEM((3, 2, nvar, halves, ny, LANES), f32),
            pltpu.VMEM((2, halves, nx, LANES), f32),
            pltpu.VMEM((2, nvar, halves, nx, LANES), f32),
            pltpu.VMEM((3 * lines, nx * ny), jnp.bfloat16),
            pltpu.VMEM((NDES // (rows * LANES), rows, LANES), f32),
            pltpu.VMEM((devices, rows, LANES), f32),
            pltpu.SemaphoreType.DMA((2,)),
            pltpu.SemaphoreType.DMA((4,)),
            pltpu.SemaphoreType.DMA((nvar, halves)),
            pltpu.SemaphoreType.DMA((2, nx)),
            pltpu.SemaphoreType.DMA((3, 2, 2)),
            pltpu.SemaphoreType.DMA((3, 2, 2)),
            pltpu.SemaphoreType.DMA((2,)),
            pltpu.SemaphoreType.REGULAR((rounds,)),
        ],
        compiler_params=pltpu.CompilerParams(
            collective_id=0, has_side_effects=True, vmem_limit_bytes=grant
        ),
    )(
        adjoint,
        objective_gradient,
        diagonal,
        jnp.transpose(flux_blocks, (2, 3, 0, 1)),
        flux_sensitivity,
        surface_mask,
        patch_band_slot,
        design_basis,
        condition_weights,
    )
    smoothed, residual, gradient = pl.pallas_call(
        write,
        out_shape=(
            jax.ShapeDtypeStruct(adjoint.shape, f32),
            jax.ShapeDtypeStruct(adjoint.shape, f32),
            jax.ShapeDtypeStruct((rows, LANES), f32),
        ),
        in_specs=[vmem] * 3,
        out_specs=(hbm, hbm, hbm),
        scratch_shapes=[pltpu.SemaphoreType.DMA((2 + halves,))],
        compiler_params=pltpu.CompilerParams(vmem_limit_bytes=2**20),
    )(smoothed, residual, gradient)
    flat = gradient.reshape(-1)
    if per_owner < flat.shape[0]:
        owner = lax.axis_index(("gx", "yz"))
        flat = lax.dynamic_slice_in_dim(flat, (owner * per_owner) % flat.shape[0], per_owner, 0)
    return smoothed, residual, flat


def solution(mesh):
    placed = (
        P("cond", None, "gx", "yz", None),
        P("cond", None, "gx", "yz", None),
        P("gx", "yz", None),
        P("cond", None, None, None),
        P("cond", None, "gx", "yz", None),
        P("gx", "yz", None),
        P("gx", "yz"),
        P(),
        P(),
    )
    return jax.shard_map(
        local,
        mesh=mesh,
        in_specs=placed,
        out_specs=(
            P("cond", None, "gx", "yz", None),
            P("cond", None, "gx", "yz", None),
            P(("gx", "yz")),
        ),
        check_vma=False,
    )
```

```python
import functools

import jax
import jax.numpy as jnp
from jax import lax
from jax.experimental import pallas as pl
from jax.experimental.pallas import tpu as pltpu
from jax.sharding import PartitionSpec as P

NDES = 4096
RELAX = 0.8
LANES = 128
PAD = 8
MESH = pl.DeviceIdType.MESH


def spans_of(count):
    reach, out = 1, []
    while reach < count - 1:
        out.append(reach)
        reach *= 2
    return out


def kernel(
    sizes,
    adjoint,
    source_hbm,
    diagonal_hbm,
    flux_hbm,
    sensitivity_hbm,
    mask_hbm,
    slots_hbm,
    basis_hbm,
    weights_hbm,
    smoothed_out,
    residual_out,
    gradient_out,
    first,
    second,
    source,
    step_of,
    bands,
    parts,
    products,
    flux,
    sensitivity,
    mask,
    slots,
    basis,
    weights,
    surface,
    edges,
    row_true,
    face_sent,
    row_halo,
    face_halo,
    corner,
    row_more,
    face_more,
    step_edge,
    weight_edge,
    onehot,
    pieces,
    arrived,
    scalar_sems,
    local_sems,
    adjoint_sems,
    plane_sems,
    row_sems,
    face_sems,
    corner_sems,
    piece_sems,
    round_sems,
):
    n_cond, n_gx, n_yz = sizes
    devices = n_cond * n_gx * n_yz
    nvar, nx, ny, nz = source.shape
    block = nvar * ny
    rows = pieces.shape[1]
    per_owner = NDES // (n_gx * n_yz)
    lines = NDES // LANES
    ci, xi, yi = lax.axis_index("cond"), lax.axis_index("gx"), lax.axis_index("yz")
    me = (ci * n_gx + xi) * n_yz + yi
    has_before_x, has_after_x = xi > 0, xi < n_gx - 1
    has_before_y, has_after_y = yi > 0, yi < n_yz - 1
    after_x, before_x = (ci, xi + 1, yi), (ci, xi - 1, yi)
    after_y, before_y = (ci, xi, yi + 1), (ci, xi, yi - 1)

    def signal(sem, target):
        pl.semaphore_signal(sem, inc=1, device_id=target, device_id_type=MESH)

    barrier = pltpu.get_barrier_semaphore()
    around = [
        (has_before_x, before_x),
        (has_after_x, after_x),
        (has_before_y, before_y),
        (has_after_y, after_y),
    ]
    diagonals = []
    for xs, there_x in ((-1, has_before_x), (1, has_after_x)):
        for ys, there_y in ((-1, has_before_y), (1, has_after_y)):
            diagonals.append((jnp.logical_and(there_x, there_y), (ci, xi + xs, yi + ys)))
    beside = n_cond - 1
    for there, target in around + diagonals:
        pl.when(there)(functools.partial(signal, barrier, target))
        beside = beside + there.astype(jnp.int32)
    for t in range(1, n_cond):
        signal(barrier, ((ci + t) % n_cond, xi, yi))

    scalar_loads = [
        pltpu.make_async_copy(flux_hbm, flux, scalar_sems.at[0]),
        pltpu.make_async_copy(weights_hbm, weights, scalar_sems.at[1]),
    ]
    adjoint_loads = [
        pltpu.make_async_copy(adjoint.at[0, :, x], first.at[pl.ds(0, nvar), x], adjoint_sems.at[x])
        for x in range(nx)
    ]
    adjoint_loads.append(pltpu.make_async_copy(diagonal_hbm, first.at[nvar], adjoint_sems.at[nx]))

    source_loads = [
        pltpu.make_async_copy(source_hbm.at[0, :, x], source.at[:, x], plane_sems.at[x])
        for x in range(nx)
    ]

    late_loads = [
        pltpu.make_async_copy(src, dst, local_sems.at[i])
        for i, (src, dst) in enumerate(
            (
                (sensitivity_hbm.at[0], sensitivity),
                (mask_hbm, mask),
                (slots_hbm, slots),
                (basis_hbm, basis),
            )
        )
    ]
    for copy in scalar_loads + adjoint_loads + source_loads + late_loads:
        copy.start()

    def field(stage):
        return smoothed_out.at[0] if stage == 2 else (first, second)[stage]

    def clear_face(side):
        for stage in range(3):
            face_halo[stage, side] = jnp.zeros((nvar + 1, ny, nz), jnp.float32)
        face_halo[0, side, nvar] = jnp.ones((ny, nz), jnp.float32)

    def clear_row(side):
        for stage in range(3):
            row_halo[stage, side] = jnp.zeros((nvar + 1, nx, nz), jnp.float32)
        row_halo[0, side, nvar] = jnp.ones((nx, nz), jnp.float32)

    def clear_corner(i):
        corner[:, i : i + 1, :] = jnp.zeros((nvar, 1, nz), jnp.float32)

    corner[:, 4:, :] = jnp.zeros((nvar, 4, nz), jnp.float32)
    for i, (there, _) in enumerate(diagonals):
        pl.when(jnp.logical_not(there))(functools.partial(clear_corner, i))
    pl.when(xi == 0)(functools.partial(clear_face, 0))
    pl.when(xi == n_gx - 1)(functools.partial(clear_face, 1))
    pl.when(yi == 0)(functools.partial(clear_row, 0))
    pl.when(yi == n_yz - 1)(functools.partial(clear_row, 1))
    depth = parts.shape[1]
    if depth > 3 * block:
        for x in range(nx):
            parts[x, 3 * block :] = jnp.zeros((depth - 3 * block, nz), jnp.bfloat16)

    def remote(src, dst, sems, target):
        return pltpu.make_async_remote_copy(
            src_ref=src,
            dst_ref=dst,
            send_sem=sems[0],
            recv_sem=sems[1],
            device_id=target,
            device_id_type=MESH,
        )

    def copies(stage):
        sent = pl.ds(0, nvar + 1 if stage == 0 else nvar)

        def face(side, x):
            return face_sent.at[side] if stage == 1 else field(stage).at[:, x]

        def sems(ref, way):
            return ref.at[stage, 0, way], ref.at[stage, 1, way]

        def into(ref, side):
            return ref.at[stage, side, sent]

        up_x = remote(face(1, nx - 1), into(face_halo, 0), sems(face_sems, 0), after_x)
        down_x = remote(face(0, 0), into(face_halo, 1), sems(face_sems, 1), before_x)
        up_y = remote(edges.at[stage, 1, sent], into(row_halo, 0), sems(row_sems, 0), after_y)
        down_y = remote(edges.at[stage, 0, sent], into(row_halo, 1), sems(row_sems, 1), before_y)
        return (
            [(has_after_x, has_before_x, up_x), (has_before_x, has_after_x, down_x)],
            [(has_after_y, has_before_y, up_y), (has_before_y, has_after_y, down_y)],
        )

    corner_copies = []
    for i, (there, target) in enumerate(diagonals):
        x, side = (0, nx - 1)[i // 2], i % 2
        copy = remote(
            edges.at[0, side, pl.ds(0, nvar), pl.ds(x, 1), :],
            corner.at[:, pl.ds(3 - i, 1), :],
            (corner_sems.at[0, i], corner_sems.at[1, i]),
            target,
        )
        corner_copies.append((there, diagonals[3 - i][0], copy))

    def begin(plans):
        for go, _, copy in plans:
            pl.when(go)(copy.start)

    def receive(plans):
        for _, come, copy in plans:
            pl.when(come)(copy.wait_recv)

    def drain(plans):
        for go, _, copy in plans:
            pl.when(go)(copy.wait_send)

    def line_round(distances):
        targets = []
        for axis, distance in distances:
            here, count = (xi, n_gx) if axis == "gx" else (yi, n_yz)
            for sign in (1, -1):
                there = here + sign * distance
                target = (ci, there, yi) if axis == "gx" else (ci, xi, there)
                targets.append((jnp.logical_and(there >= 0, there < count), target))
        return targets

    gx_spans, yz_spans = spans_of(n_gx), spans_of(n_yz)
    rounds = []
    for i in range(max(len(gx_spans), len(yz_spans))):
        distances = [("gx", d) for d in gx_spans[i : i + 1]] + [("yz", d) for d in yz_spans[i : i + 1]]
        rounds.append(line_round(distances))
    always = ci >= 0
    rounds.append([(always, (ci, (xi + t) % n_gx, yi)) for t in range(1, n_gx)])
    rounds.append([(always, ((ci + t) % n_cond, xi, yi)) for t in range(1, n_cond)])

    def tell(i):
        for there, target in rounds[i]:
            pl.when(there)(functools.partial(signal, round_sems.at[i], target))

    def hear(i):
        count = 0
        for there, _ in rounds[i]:
            count = count + there.astype(jnp.int32)
        pl.semaphore_wait(round_sems.at[i], count)

    def advance(i):
        hear(i)
        if i + 1 < len(rounds):
            tell(i + 1)

    def keep_edges(kept, k, x, value):
        kept[0, k, x : x + 1, :] = value[0:1]
        kept[1, k, x : x + 1, :] = value[ny - 1 : ny]

    def rows_of(stage):
        return row_true if stage == 1 else edges.at[stage]

    def split(value):
        high = value.astype(jnp.bfloat16)
        return high, (value - high.astype(jnp.float32)).astype(jnp.bfloat16)

    column = lax.broadcasted_iota(jnp.int32, (ny, depth), 1)
    row = lax.broadcasted_iota(jnp.int32, (ny, depth), 0)
    part = column // block
    pair = column - part * block
    from_var = pair // ny
    offset = pair - from_var * ny - row

    for copy in scalar_loads:
        copy.wait()

    def spread(k, d):
        total = jnp.zeros((ny, depth), jnp.float32)
        for e in range(nvar):
            total = jnp.where(from_var == e, flux[e, k, 0, d], total)
        upper = total.astype(jnp.bfloat16).astype(jnp.float32)
        lower = (total - upper).astype(jnp.bfloat16).astype(jnp.float32)
        return jnp.where(part < 2, upper, jnp.where(part == 2, lower, 0.0))

    for k in range(nvar):
        own = jnp.where(offset == 1, spread(k, 2), jnp.where(offset == -1, spread(k, 3), 0.0))
        bands[k * ny : (k + 1) * ny, :] = own.astype(jnp.bfloat16)
        for g, d in ((1, 0), (2, 1), (3, 4), (4, 5)):
            other = jnp.where(offset == 0, spread(k, d), 0.0)
            at = g * block + k * ny
            bands[at : at + ny, :] = other.astype(jnp.bfloat16)

    pl.semaphore_wait(barrier, beside)
    tell(0)
    for copy in adjoint_loads:
        copy.wait()
    for x in range(nx):
        for k in range(nvar + 1):
            keep_edges(edges.at[0], k, x, first[k, x])
    for plans in copies(0):
        begin(plans)
    begin(corner_copies)

    dot = functools.partial(jnp.dot, preferred_element_type=jnp.float32)
    last_lane = lax.broadcasted_iota(jnp.int32, (ny, nz), 1)

    def multiply(stage, x):
        for e in range(nvar):
            high, low = split(field(stage)[e, x])
            for p, value in enumerate((high, low, high)):
                at = p * block + e * ny
                parts[x, at : at + ny, :] = value
        products[x] = dot(bands[...], parts[x])

    def gathered(x, k):
        def product(plane, g):
            at = g * block + k * ny
            return products[plane, at : at + ny, :]

        acc = source[k, x] + product(x, 0)
        if x + 1 < nx:
            acc = acc + product(x + 1, 1)
        if x > 0:
            acc = acc + product(x - 1, 2)
        up = pltpu.roll(product(x, 3), nz - 1, 1)
        down = pltpu.roll(product(x, 4), 1, 1)
        up = jnp.where(last_lane == nz - 1, 0.0, up)
        down = jnp.where(last_lane == 0, 0.0, down)
        return acc + up + down

    def relax(stage, x):
        if stage == 0:
            step = RELAX / first[nvar, x]
            step_of[x] = step
            step_edge[0, x : x + 1, :] = step[0:1]
            step_edge[1, x : x + 1, :] = step[ny - 1 : ny]
        else:
            step = step_of[x]
            cover = mask[x].astype(jnp.float32)
        total = None
        for k in range(nvar):
            value = (1.0 - RELAX) * field(stage)[k, x] + step * gathered(x, k)
            field(stage + 1)[k, x] = value
            keep_edges(edges.at[stage + 1], k, x, value)
            if stage == 0:
                keep_edges(row_true, k, x, value)
                for side, plane in ((0, 0), (1, nx - 1)):
                    if x == plane:
                        face_sent[side, k] = value
            if stage == 1:
                weight = sensitivity[k, x].astype(jnp.float32) * cover
                weight_edge[0, k, x : x + 1, :] = weight[0:1]
                weight_edge[1, k, x : x + 1, :] = weight[ny - 1 : ny]
                term = value * weight
                total = term if k == 0 else total + term
        if stage == 1:
            surface[x] = total

    def settle(stage, x):
        for k in range(nvar):
            value = gathered(x, k) - first[nvar, x] * field(2)[k, x]
            residual_out[0, k, x] = value
            keep_edges(edges.at[3], k, x, value)

    def sweep(stage, finish, between=None):
        multiply(stage, 0)
        for x in range(nx):
            if between is not None and x == nx // 2:
                between()
            if x + 1 < nx:
                multiply(stage, x + 1)
            finish(stage, x)

    def brought(cells, d):
        out = []
        for k in range(nvar):
            total = flux[0, k, 0, d] * cells[0]
            for e in range(1, nvar):
                total = total + flux[e, k, 0, d] * cells[e]
            out.append(total)
        return out

    def halo_of(halo, more, stage, side):
        cells = [halo[stage, side, e] for e in range(nvar)]
        return [c + more[side, e] for e, c in enumerate(cells)] if stage == 1 else cells

    def add_own():
        spot = lax.broadcasted_iota(jnp.int32, (8, nz), 0)
        lines_of = [corner[e] for e in range(nvar)]
        along_x, along_y = [], []
        for k in range(nvar):
            for out, near, ds in ((along_x, spot < 2, (1, 0)), (along_y, spot % 2 == 0, (3, 2))):
                total = None
                for e in range(nvar):
                    scale = jnp.where(near, flux[e, k, 0, ds[0]], flux[e, k, 0, ds[1]])
                    term = scale * lines_of[e]
                    total = term if e == 0 else total + term
                out.append(total)
        at_row = lax.broadcasted_iota(jnp.int32, (nx, nz), 0)
        at_face = lax.broadcasted_iota(jnp.int32, (ny, nz), 0)
        for side, d, there in ((0, 2, has_before_y), (1, 3, has_after_y)):
            step = jnp.where(there, RELAX / row_halo[0, side, nvar], 0.0)
            mine = brought([edges[0, side, e] for e in range(nvar)], d)
            for k in range(nvar):
                ends = along_x[k][side : side + 1], along_x[k][2 + side : 3 + side]
                extra = jnp.where(at_row == 0, ends[0], jnp.where(at_row == nx - 1, ends[1], 0.0))
                row_more[side, k] = step * (mine[k] + extra)
        for side, x, d, there in ((0, 0, 0, has_before_x), (1, nx - 1, 1, has_after_x)):
            step = jnp.where(there, RELAX / face_halo[0, side, nvar], 0.0)
            mine = brought([first[e, x] for e in range(nvar)], d)
            for k in range(nvar):
                i = 2 * side
                ends = along_y[k][i : i + 1], along_y[k][i + 1 : i + 2]
                extra = jnp.where(at_face == 0, ends[0], jnp.where(at_face == ny - 1, ends[1], 0.0))
                face_more[side, k] = step * (mine[k] + extra)

    def add_faces(stage):
        for side, x, d in ((0, 0, 1), (1, nx - 1, 0)):
            more = brought(halo_of(face_halo, face_more, stage, side), d)
            total = None
            for k in range(nvar):
                if stage == 2:
                    value = residual_out[0, k, x] + more[k]
                    residual_out[0, k, x] = value
                else:
                    part = step_of[x] * more[k]
                    value = field(stage + 1)[k, x] + part
                    field(stage + 1)[k, x] = value
                    if stage == 1:
                        term = part * sensitivity[k, x].astype(jnp.float32)
                        total = term if k == 0 else total + term
                keep_edges(rows_of(stage + 1), k, x, value)
            if stage == 1:
                surface[x] = surface[x] + total * mask[x].astype(jnp.float32)

    def add_rows(stage):
        for side, y, d in ((0, 0, 3), (1, ny - 1, 2)):
            more = brought(halo_of(row_halo, row_more, stage, side), d)
            total = None
            for k in range(nvar):
                part = more[k] if stage == 2 else step_edge[side] * more[k]
                value = rows_of(stage + 1)[side, k] + part
                if stage == 1:
                    edges[2, side, k] = value
                if stage == 1:
                    term = part * weight_edge[side, k]
                    total = term if k == 0 else total + term
                for x in range(nx):
                    if stage == 2:
                        residual_out[0, k, x, y : y + 1, :] = value[x : x + 1]
                    else:
                        field(stage + 1)[k, x, y : y + 1, :] = value[x : x + 1]
            if stage == 1:
                for x in range(nx):
                    surface[x, y : y + 1, :] = surface[x, y : y + 1, :] + total[x : x + 1]

    def complete(stage):
        faces, ranks = copies(stage)
        receive(faces)
        add_faces(stage)
        receive(ranks)
        add_rows(stage)

    for copy in source_loads:
        copy.wait()
    advance(0)
    sweep(0, relax)
    for plans in copies(1):
        begin(plans)
    for i in range(1, len(rounds) - 2):
        advance(i)
    complete(0)
    for copy in late_loads:
        copy.wait()
    sweep(1, relax, functools.partial(advance, len(rounds) - 2))
    receive(corner_copies)
    add_own()

    line = lax.broadcasted_iota(jnp.int32, (lines, nx * ny), 0)
    spots = jnp.concatenate([slots[x : x + 1, :] for x in range(nx)], axis=1)
    wanted = jnp.concatenate([2 * line, 2 * line + 1, 2 * line - 1], axis=0)
    onehot[...] = (wanted == spots).astype(jnp.float32).astype(jnp.bfloat16)
    weight_sum = weights[0]
    for c in range(1, n_cond):
        weight_sum = weight_sum + weights[c]
    share = jnp.full((1, LANES), weights[ci], jnp.int32).astype(jnp.float32) / jnp.full(
        (1, LANES), weight_sum, jnp.int32
    ).astype(jnp.float32)

    complete(1)
    for plans in copies(2):
        begin(plans)

    basis_high, basis_low = split(basis[...])
    surface_high, surface_low = split(surface[...].reshape(nx * ny, nz))
    projected = (
        dot(surface_high, basis_high) + dot(surface_high, basis_low) + dot(surface_low, basis_high)
    )
    high, low = split(projected)
    looked = dot(onehot[...], high) + dot(onehot[...], low)
    turned = pltpu.roll(looked[lines:], LANES // 2, 1)
    spot = lax.broadcasted_iota(jnp.int32, (lines, LANES), 1)
    gradient = looked[:lines] + jnp.where(spot < LANES // 2, turned[lines:], turned[:lines])
    gradient = gradient * share
    for g in range(lines // rows):
        pieces[g] = gradient[g * rows : (g + 1) * rows]

    def group(gx, yz):
        return (gx * n_yz + yz) * per_owner // (rows * LANES)

    def give(c, gx, yz):
        remote(
            pieces.at[group(gx, yz)],
            arrived.at[me],
            (piece_sems.at[0], piece_sems.at[1]),
            (c, gx, yz),
        ).start()

    arrived[me] = pieces[group(xi, yi)]
    advance(len(rounds) - 1)
    if devices <= 64:
        for dy in range(n_yz):
            for dx in range(n_gx):
                for dc in range(n_cond):
                    if dc or dx or dy:
                        give((ci + dc) % n_cond, (xi + dx) % n_gx, (yi + dy) % n_yz)
    else:

        def give_next(t, carry):
            flat = (me + t) % devices
            give(flat // (n_gx * n_yz), (flat // n_yz) % n_gx, flat % n_yz)
            return carry

        lax.fori_loop(1, devices, give_next, 0)

    sweep(2, settle)
    others = arrived.at[pl.ds(0, devices - 1)]
    for i in range(2):
        pltpu.make_async_copy(others, others, piece_sems.at[i]).wait()
    gradient_out[...] = jnp.sum(arrived[...], axis=0)
    complete(2)
    for stage in range(3):
        for plans in copies(stage):
            drain(plans)
    drain(corner_copies)


def write(smoothed, residual, gradient, smoothed_hbm, residual_hbm, gradient_hbm, sems):
    stores = [
        pltpu.make_async_copy(src, dst, sems.at[i])
        for i, (src, dst) in enumerate(
            ((smoothed, smoothed_hbm), (residual, residual_hbm), (gradient, gradient_hbm))
        )
    ]
    for copy in stores:
        copy.start()
    for copy in stores:
        copy.wait()


def local(
    adjoint,
    objective_gradient,
    diagonal,
    flux_blocks,
    flux_sensitivity,
    surface_mask,
    patch_band_slot,
    design_basis,
    condition_weights,
):
    sizes = tuple(lax.axis_size(axis) for axis in ("cond", "gx", "yz"))
    devices = sizes[0] * sizes[1] * sizes[2]
    _, nvar, nx, ny, nz = adjoint.shape
    per_owner = NDES // (sizes[1] * sizes[2])
    rows = max(1, per_owner // LANES)
    lines = NDES // LANES
    rounds = max(len(spans_of(sizes[1])), len(spans_of(sizes[2]))) + 2
    f32 = jnp.float32
    hbm = pl.BlockSpec(memory_space=pltpu.MemorySpace.HBM)
    vmem = pl.BlockSpec(memory_space=pltpu.MemorySpace.VMEM)
    depth = -(-3 * nvar * ny // (2 * LANES)) * 2 * LANES
    grant = 67043328 - 2**16 - 2 * adjoint.size * 4
    smoothed, residual, gradient = pl.pallas_call(
        functools.partial(kernel, sizes),
        out_shape=(
            pltpu.VMEM(adjoint.shape, f32),
            pltpu.VMEM(adjoint.shape, f32),
            pltpu.VMEM((rows, LANES), f32),
        ),
        in_specs=[hbm] * 9,
        out_specs=(vmem, vmem, vmem),
        scratch_shapes=[
            pltpu.VMEM((nvar + 1, nx, ny, nz), f32),
            pltpu.VMEM((nvar, nx, ny, nz), f32),
            pltpu.VMEM((nvar, nx, ny, nz), f32),
            pltpu.VMEM((nx, ny, nz), f32),
            pltpu.VMEM((5 * nvar * ny, depth), jnp.bfloat16),
            pltpu.VMEM((nx, depth, nz), jnp.bfloat16),
            pltpu.VMEM((nx, 5 * nvar * ny, nz), f32),
            pltpu.SMEM((nvar, nvar, 1, 6), f32),
            pltpu.VMEM((nvar, nx, ny, nz), jnp.bfloat16),
            pltpu.VMEM((nx, ny, nz), jnp.int32),
            pltpu.VMEM((nx, ny), jnp.int32),
            pltpu.VMEM(design_basis.shape, f32),
            pltpu.SMEM(condition_weights.shape, jnp.int32),
            pltpu.VMEM((nx, ny, nz), f32),
            pltpu.VMEM((4, 2, nvar + 1, nx, nz), f32),
            pltpu.VMEM((2, nvar, nx, nz), f32),
            pltpu.VMEM((2, nvar, ny, nz), f32),
            pltpu.VMEM((3, 2, nvar + 1, nx, nz), f32),
            pltpu.VMEM((3, 2, nvar + 1, ny, nz), f32),
            pltpu.VMEM((nvar, 8, nz), f32),
            pltpu.VMEM((2, nvar, nx, nz), f32),
            pltpu.VMEM((2, nvar, ny, nz), f32),
            pltpu.VMEM((2, nx, nz), f32),
            pltpu.VMEM((2, nvar, nx, nz), f32),
            pltpu.VMEM((3 * lines, nx * ny), jnp.bfloat16),
            pltpu.VMEM((NDES // (rows * LANES), rows, LANES), f32),
            pltpu.VMEM((devices, rows, LANES), f32),
            pltpu.SemaphoreType.DMA((2,)),
            pltpu.SemaphoreType.DMA((4,)),
            pltpu.SemaphoreType.DMA((nx + 1,)),
            pltpu.SemaphoreType.DMA((nx,)),
            pltpu.SemaphoreType.DMA((3, 2, 2)),
            pltpu.SemaphoreType.DMA((3, 2, 2)),
            pltpu.SemaphoreType.DMA((2, 4)),
            pltpu.SemaphoreType.DMA((2,)),
            pltpu.SemaphoreType.REGULAR((rounds,)),
        ],
        compiler_params=pltpu.CompilerParams(
            collective_id=0, has_side_effects=True, vmem_limit_bytes=grant
        ),
    )(
        adjoint,
        objective_gradient,
        diagonal,
        jnp.transpose(flux_blocks, (2, 3, 0, 1)),
        flux_sensitivity,
        surface_mask,
        patch_band_slot,
        design_basis,
        condition_weights,
    )
    smoothed, residual, gradient = pl.pallas_call(
        write,
        out_shape=(
            jax.ShapeDtypeStruct(adjoint.shape, f32),
            jax.ShapeDtypeStruct(adjoint.shape, f32),
            jax.ShapeDtypeStruct((rows, LANES), f32),
        ),
        in_specs=[vmem] * 3,
        out_specs=(hbm, hbm, hbm),
        scratch_shapes=[pltpu.SemaphoreType.DMA((3,))],
        compiler_params=pltpu.CompilerParams(vmem_limit_bytes=2**20),
    )(smoothed, residual, gradient)
    flat = gradient.reshape(-1)
    if per_owner < flat.shape[0]:
        owner = lax.axis_index(("gx", "yz"))
        flat = lax.dynamic_slice_in_dim(flat, (owner * per_owner) % flat.shape[0], per_owner, 0)
    return smoothed, residual, flat


def solution(mesh):
    placed = (
        P("cond", None, "gx", "yz", None),
        P("cond", None, "gx", "yz", None),
        P("gx", "yz", None),
        P("cond", None, None, None),
        P("cond", None, "gx", "yz", None),
        P("gx", "yz", None),
        P("gx", "yz"),
        P(),
        P(),
    )
    return jax.shard_map(
        local,
        mesh=mesh,
        in_specs=placed,
        out_specs=(
            P("cond", None, "gx", "yz", None),
            P("cond", None, "gx", "yz", None),
            P(("gx", "yz")),
        ),
        check_vma=False,
    )
```

```python
import functools

import jax
import jax.numpy as jnp
from jax import lax
from jax.experimental import pallas as pl
from jax.experimental.pallas import tpu as pltpu
from jax.sharding import PartitionSpec as P

NDES = 4096
RELAX = 0.8
LANES = 128
PAD = 8
MESH = pl.DeviceIdType.MESH


def spans_of(count):
    reach, out = 1, []
    while reach < count - 1:
        out.append(reach)
        reach *= 2
    return out


def kernel(
    sizes,
    adjoint,
    source_hbm,
    diagonal_hbm,
    flux_hbm,
    sensitivity_hbm,
    mask_hbm,
    slots_hbm,
    basis_hbm,
    weights_hbm,
    smoothed_out,
    residual_out,
    gradient_out,
    first,
    second,
    source,
    step_of,
    bands,
    parts,
    products,
    flux,
    sensitivity,
    mask,
    slots,
    basis,
    weights,
    surface,
    edges,
    row_true,
    face_sent,
    row_halo,
    face_halo,
    corner,
    row_more,
    face_more,
    step_edge,
    weight,
    weight_edge,
    basis_parts,
    onehot,
    pieces,
    arrived,
    scalar_sems,
    local_sems,
    early_sems,
    row_sems,
    face_sems,
    corner_sems,
    diagonal_sems,
    piece_sems,
    round_sems,
):
    n_cond, n_gx, n_yz = sizes
    devices = n_cond * n_gx * n_yz
    nvar, nx, ny, nz = source.shape
    block = nvar * ny
    rows = pieces.shape[1]
    per_owner = NDES // (n_gx * n_yz)
    lines = NDES // LANES
    ci, xi, yi = lax.axis_index("cond"), lax.axis_index("gx"), lax.axis_index("yz")
    me = (ci * n_gx + xi) * n_yz + yi
    has_before_x, has_after_x = xi > 0, xi < n_gx - 1
    has_before_y, has_after_y = yi > 0, yi < n_yz - 1
    after_x, before_x = (ci, xi + 1, yi), (ci, xi - 1, yi)
    after_y, before_y = (ci, xi, yi + 1), (ci, xi, yi - 1)

    def signal(sem, target):
        pl.semaphore_signal(sem, inc=1, device_id=target, device_id_type=MESH)

    barrier = pltpu.get_barrier_semaphore()
    around = [
        (has_before_x, before_x),
        (has_after_x, after_x),
        (has_before_y, before_y),
        (has_after_y, after_y),
    ]
    diagonals = []
    for xs, there_x in ((-1, has_before_x), (1, has_after_x)):
        for ys, there_y in ((-1, has_before_y), (1, has_after_y)):
            diagonals.append((jnp.logical_and(there_x, there_y), (ci, xi + xs, yi + ys)))
    beside = n_cond - 1
    for there, target in around + diagonals:
        pl.when(there)(functools.partial(signal, barrier, target))
        beside = beside + there.astype(jnp.int32)
    for t in range(1, n_cond):
        signal(barrier, ((ci + t) % n_cond, xi, yi))

    scalar_loads = [
        pltpu.make_async_copy(flux_hbm, flux, scalar_sems.at[0]),
        pltpu.make_async_copy(weights_hbm, weights, scalar_sems.at[1]),
    ]
    adjoint_loads = [
        pltpu.make_async_copy(adjoint.at[0], first.at[pl.ds(0, nvar)], early_sems.at[0]),
        pltpu.make_async_copy(diagonal_hbm, first.at[nvar], early_sems.at[1]),
    ]
    source_loads = [pltpu.make_async_copy(source_hbm.at[0], source, early_sems.at[2])]

    late_loads = [
        pltpu.make_async_copy(src, dst, local_sems.at[i])
        for i, (src, dst) in enumerate(
            (
                (sensitivity_hbm.at[0], sensitivity),
                (mask_hbm, mask),
                (slots_hbm, slots),
                (basis_hbm, basis),
            )
        )
    ]
    for copy in scalar_loads + adjoint_loads + source_loads + late_loads:
        copy.start()

    def field(stage):
        return smoothed_out.at[0] if stage == 2 else (first, second)[stage]

    def clear_face(side):
        for stage in range(3):
            face_halo[stage, side] = jnp.zeros((nvar + 1, ny, nz), jnp.float32)
        face_halo[0, side, nvar] = jnp.ones((ny, nz), jnp.float32)

    def clear_row(side):
        for stage in range(3):
            row_halo[stage, side] = jnp.zeros((nvar + 1, nx, nz), jnp.float32)
        row_halo[0, side, nvar] = jnp.ones((nx, nz), jnp.float32)

    def clear_corner(i):
        corner[:, i : i + 1, :] = jnp.zeros((nvar, 1, nz), jnp.float32)

    corner[:, 4:, :] = jnp.zeros((nvar, 4, nz), jnp.float32)
    for i, (there, _) in enumerate(diagonals):
        pl.when(jnp.logical_not(there))(functools.partial(clear_corner, i))
    pl.when(xi == 0)(functools.partial(clear_face, 0))
    pl.when(xi == n_gx - 1)(functools.partial(clear_face, 1))
    pl.when(yi == 0)(functools.partial(clear_row, 0))
    pl.when(yi == n_yz - 1)(functools.partial(clear_row, 1))
    depth = parts.shape[1]
    if depth > 3 * block:
        for x in range(nx):
            parts[x, 3 * block :] = jnp.zeros((depth - 3 * block, nz), jnp.bfloat16)

    def remote(src, dst, sems, target):
        return pltpu.make_async_remote_copy(
            src_ref=src,
            dst_ref=dst,
            send_sem=sems[0],
            recv_sem=sems[1],
            device_id=target,
            device_id_type=MESH,
        )

    def copies(stage):
        sent = pl.ds(0, nvar)

        def face(side, x):
            return face_sent.at[side] if stage == 1 else field(stage).at[sent, x]

        def sems(ref, way):
            return ref.at[stage, 0, way], ref.at[stage, 1, way]

        def into(ref, side):
            return ref.at[stage, side, sent]

        up_x = remote(face(1, nx - 1), into(face_halo, 0), sems(face_sems, 0), after_x)
        down_x = remote(face(0, 0), into(face_halo, 1), sems(face_sems, 1), before_x)
        up_y = remote(edges.at[stage, 1, sent], into(row_halo, 0), sems(row_sems, 0), after_y)
        down_y = remote(edges.at[stage, 0, sent], into(row_halo, 1), sems(row_sems, 1), before_y)
        return (
            [(has_after_x, has_before_x, up_x), (has_before_x, has_after_x, down_x)],
            [(has_after_y, has_before_y, up_y), (has_before_y, has_after_y, down_y)],
        )

    def diagonal_copies():
        def sems(way):
            return diagonal_sems.at[0, way], diagonal_sems.at[1, way]

        up_x = remote(first.at[nvar, nx - 1], face_halo.at[0, 0, nvar], sems(0), after_x)
        down_x = remote(first.at[nvar, 0], face_halo.at[0, 1, nvar], sems(1), before_x)
        up_y = remote(edges.at[0, 1, nvar], row_halo.at[0, 0, nvar], sems(2), after_y)
        down_y = remote(edges.at[0, 0, nvar], row_halo.at[0, 1, nvar], sems(3), before_y)
        return [
            (has_after_x, has_before_x, up_x),
            (has_before_x, has_after_x, down_x),
            (has_after_y, has_before_y, up_y),
            (has_before_y, has_after_y, down_y),
        ]

    corner_copies = []
    for i, (there, target) in enumerate(diagonals):
        x, side = (0, nx - 1)[i // 2], i % 2
        copy = remote(
            edges.at[0, side, pl.ds(0, nvar), pl.ds(x, 1), :],
            corner.at[:, pl.ds(3 - i, 1), :],
            (corner_sems.at[0, i], corner_sems.at[1, i]),
            target,
        )
        corner_copies.append((there, diagonals[3 - i][0], copy))

    def begin(plans):
        for go, _, copy in plans:
            pl.when(go)(copy.start)

    def receive(plans):
        for _, come, copy in plans:
            pl.when(come)(copy.wait_recv)

    def drain(plans):
        for go, _, copy in plans:
            pl.when(go)(copy.wait_send)

    def line_round(distances):
        targets = []
        for axis, distance in distances:
            here, count = (xi, n_gx) if axis == "gx" else (yi, n_yz)
            for sign in (1, -1):
                there = here + sign * distance
                target = (ci, there, yi) if axis == "gx" else (ci, xi, there)
                targets.append((jnp.logical_and(there >= 0, there < count), target))
        return targets

    gx_spans, yz_spans = spans_of(n_gx), spans_of(n_yz)
    rounds = []
    for i in range(max(len(gx_spans), len(yz_spans))):
        distances = [("gx", d) for d in gx_spans[i : i + 1]] + [("yz", d) for d in yz_spans[i : i + 1]]
        rounds.append(line_round(distances))
    always = ci >= 0
    rounds.append([(always, (ci, (xi + t) % n_gx, yi)) for t in range(1, n_gx)])
    rounds.append([(always, ((ci + t) % n_cond, xi, yi)) for t in range(1, n_cond)])

    def tell(i):
        for there, target in rounds[i]:
            pl.when(there)(functools.partial(signal, round_sems.at[i], target))

    def hear(i):
        count = 0
        for there, _ in rounds[i]:
            count = count + there.astype(jnp.int32)
        pl.semaphore_wait(round_sems.at[i], count)

    def advance(i):
        hear(i)
        if i + 1 < len(rounds):
            tell(i + 1)

    def keep_edges(kept, k, x, value):
        kept[0, k, x : x + 1, :] = value[0:1]
        kept[1, k, x : x + 1, :] = value[ny - 1 : ny]

    def rows_of(stage):
        return row_true if stage == 1 else edges.at[stage]

    def split(value):
        high = value.astype(jnp.bfloat16)
        return high, (value - high.astype(jnp.float32)).astype(jnp.bfloat16)

    column = lax.broadcasted_iota(jnp.int32, (ny, depth), 1)
    row = lax.broadcasted_iota(jnp.int32, (ny, depth), 0)
    part = column // block
    pair = column - part * block
    from_var = pair // ny
    offset = pair - from_var * ny - row

    for copy in scalar_loads:
        copy.wait()

    def spread(k, d):
        total = jnp.zeros((ny, depth), jnp.float32)
        for e in range(nvar):
            total = jnp.where(from_var == e, flux[e, k, 0, d], total)
        upper = total.astype(jnp.bfloat16).astype(jnp.float32)
        lower = (total - upper).astype(jnp.bfloat16).astype(jnp.float32)
        return jnp.where(part < 2, upper, jnp.where(part == 2, lower, 0.0))

    for k in range(nvar):
        own = jnp.where(offset == 1, spread(k, 2), jnp.where(offset == -1, spread(k, 3), 0.0))
        bands[k * ny : (k + 1) * ny, :] = own.astype(jnp.bfloat16)
        for g, d in ((1, 0), (2, 1), (3, 4), (4, 5)):
            other = jnp.where(offset == 0, spread(k, d), 0.0)
            at = g * block + k * ny
            bands[at : at + ny, :] = other.astype(jnp.bfloat16)

    pl.semaphore_wait(barrier, beside)
    tell(0)
    for copy in adjoint_loads:
        copy.wait()
    for x in range(nx):
        for k in range(nvar + 1):
            keep_edges(edges.at[0], k, x, first[k, x])
    for plans in copies(0):
        begin(plans)
    begin(corner_copies)
    begin(diagonal_copies())

    dot = functools.partial(jnp.dot, preferred_element_type=jnp.float32)
    lane = lax.broadcasted_iota(jnp.int32, (ny, LANES), 1)
    spans = [slice(h * LANES, (h + 1) * LANES) for h in range(nz // LANES)]

    def multiply(stage, x):
        for e in range(nvar):
            high, low = split(field(stage)[e, x])
            for p, value in enumerate((high, low, high)):
                at = p * block + e * ny
                parts[x, at : at + ny, :] = value
        products[x] = dot(bands[...], parts[x])

    def gathered(x, k):
        def product(plane, g):
            at = g * block + k * ny
            return products[plane, at : at + ny, :]

        acc = source[k, x] + product(x, 0)
        if x + 1 < nx:
            acc = acc + product(x + 1, 1)
        if x > 0:
            acc = acc + product(x - 1, 2)
        ahead = [pltpu.roll(product(x, 3)[:, c], LANES - 1, 1) for c in spans] + [0.0]
        behind = [0.0] + [pltpu.roll(product(x, 4)[:, c], 1, 1) for c in spans]
        shifted = [
            jnp.where(lane == LANES - 1, ahead[h + 1], ahead[h])
            + jnp.where(lane == 0, behind[h], behind[h + 1])
            for h in range(len(spans))
        ]
        return acc + jnp.concatenate(shifted, axis=1)

    def relax(stage, x):
        if stage == 0:
            step = RELAX / first[nvar, x]
            step_of[x] = step
            step_edge[0, x : x + 1, :] = step[0:1]
            step_edge[1, x : x + 1, :] = step[ny - 1 : ny]
        else:
            step = step_of[x]
        total = None
        for k in range(nvar):
            value = (1.0 - RELAX) * field(stage)[k, x] + step * gathered(x, k)
            field(stage + 1)[k, x] = value
            keep_edges(edges.at[stage + 1], k, x, value)
            if stage == 0:
                keep_edges(row_true, k, x, value)
                for side, plane in ((0, 0), (1, nx - 1)):
                    if x == plane:
                        face_sent[side, k] = value
            if stage == 1:
                term = value * weight[k, x]
                total = term if k == 0 else total + term
        if stage == 1:
            surface[x] = total

    def settle(stage, x):
        for k in range(nvar):
            value = gathered(x, k) - first[nvar, x] * field(2)[k, x]
            residual_out[0, k, x] = value
            keep_edges(edges.at[3], k, x, value)

    def sweep(stage, finish):
        multiply(stage, 0)
        for x in range(nx):
            if x + 1 < nx:
                multiply(stage, x + 1)
            finish(stage, x)

    def brought(cells, d):
        out = []
        for k in range(nvar):
            total = flux[0, k, 0, d] * cells[0]
            for e in range(1, nvar):
                total = total + flux[e, k, 0, d] * cells[e]
            out.append(total)
        return out

    def halo_of(halo, more, stage, side):
        cells = [halo[stage, side, e] for e in range(nvar)]
        return [c + more[side, e] for e, c in enumerate(cells)] if stage == 1 else cells

    def begin_own():
        for side, d in ((0, 2), (1, 3)):
            mine = brought([edges[0, side, e] for e in range(nvar)], d)
            for k in range(nvar):
                row_more[side, k] = mine[k]
        for side, x, d in ((0, 0, 0), (1, nx - 1, 1)):
            mine = brought([first[e, x] for e in range(nvar)], d)
            for k in range(nvar):
                face_more[side, k] = mine[k]

    def add_corners():
        spot = lax.broadcasted_iota(jnp.int32, (8, nz), 0)
        lines_of = [corner[e] for e in range(nvar)]
        at_row = lax.broadcasted_iota(jnp.int32, (nx, nz), 0)
        at_face = lax.broadcasted_iota(jnp.int32, (ny, nz), 0)
        for k in range(nvar):
            along = []
            for near, ds in ((spot < 2, (1, 0)), (spot % 2 == 0, (3, 2))):
                total = None
                for e in range(nvar):
                    scale = jnp.where(near, flux[e, k, 0, ds[0]], flux[e, k, 0, ds[1]])
                    term = scale * lines_of[e]
                    total = term if e == 0 else total + term
                along.append(total)
            for side in range(2):
                ends = along[0][side : side + 1], along[0][2 + side : 3 + side]
                extra = jnp.where(at_row == 0, ends[0], jnp.where(at_row == nx - 1, ends[1], 0.0))
                row_more[side, k] = row_more[side, k] + extra
                ends = along[1][2 * side : 2 * side + 1], along[1][2 * side + 1 : 2 * side + 2]
                extra = jnp.where(at_face == 0, ends[0], jnp.where(at_face == ny - 1, ends[1], 0.0))
                face_more[side, k] = face_more[side, k] + extra

    def scale_more():
        for side, there in ((0, has_before_y), (1, has_after_y)):
            step = jnp.where(there, RELAX / row_halo[0, side, nvar], 0.0)
            for k in range(nvar):
                row_more[side, k] = step * row_more[side, k]
        for side, there in ((0, has_before_x), (1, has_after_x)):
            step = jnp.where(there, RELAX / face_halo[0, side, nvar], 0.0)
            for k in range(nvar):
                face_more[side, k] = step * face_more[side, k]

    def add_faces(stage):
        for side, x, d in ((0, 0, 1), (1, nx - 1, 0)):
            more = brought(halo_of(face_halo, face_more, stage, side), d)
            total = None
            for k in range(nvar):
                if stage == 2:
                    value = residual_out[0, k, x] + more[k]
                    residual_out[0, k, x] = value
                else:
                    part = step_of[x] * more[k]
                    value = field(stage + 1)[k, x] + part
                    field(stage + 1)[k, x] = value
                    if stage == 1:
                        term = part * weight[k, x]
                        total = term if k == 0 else total + term
                keep_edges(rows_of(stage + 1), k, x, value)
            if stage == 1:
                surface[x] = surface[x] + total

    def put_row(stage, k, y, value):
        for x in range(nx):
            if stage == 2:
                residual_out[0, k, x, y : y + 1, :] = value[x : x + 1]
            else:
                field(stage + 1)[k, x, y : y + 1, :] = value[x : x + 1]

    def add_rows(stage):
        for side, y, d in ((0, 0, 3), (1, ny - 1, 2)):
            more = brought(halo_of(row_halo, row_more, stage, side), d)
            total = None
            for k in range(nvar):
                part = more[k] if stage == 2 else step_edge[side] * more[k]
                value = rows_of(stage + 1)[side, k] + part
                if stage == 1:
                    edges[2, side, k] = value
                if stage == 1:
                    term = part * weight_edge[side, k]
                    total = term if k == 0 else total + term
                if stage != 1:
                    put_row(stage, k, y, value)
            if stage == 1:
                for x in range(nx):
                    surface[x, y : y + 1, :] = surface[x, y : y + 1, :] + total[x : x + 1]

    def complete(stage):
        faces, ranks = copies(stage)
        receive(faces)
        add_faces(stage)
        receive(ranks)
        add_rows(stage)

    for copy in source_loads:
        copy.wait()
    advance(0)
    sweep(0, relax)
    for plans in copies(1):
        begin(plans)
    begin_own()
    for copy in late_loads:
        copy.wait()
    for x in range(nx):
        cover = mask[x].astype(jnp.float32)
        for k in range(nvar):
            value = sensitivity[k, x].astype(jnp.float32) * cover
            weight[k, x] = value
            keep_edges(weight_edge, k, x, value)
    basis_parts[0], basis_parts[1] = split(basis[...])
    line = lax.broadcasted_iota(jnp.int32, (lines, nx * ny), 0)
    spots = jnp.concatenate([slots[x : x + 1, :] for x in range(nx)], axis=1)
    wanted = jnp.concatenate([2 * line, 2 * line + 1, 2 * line - 1], axis=0)
    onehot[...] = (wanted == spots).astype(jnp.float32).astype(jnp.bfloat16)
    for i in range(1, len(rounds) - 2):
        advance(i)
    complete(0)
    advance(len(rounds) - 2)
    receive(corner_copies)
    add_corners()
    sweep(1, relax)
    weight_sum = weights[0]
    for c in range(1, n_cond):
        weight_sum = weight_sum + weights[c]
    share = jnp.full((1, LANES), weights[ci], jnp.int32).astype(jnp.float32) / jnp.full(
        (1, LANES), weight_sum, jnp.int32
    ).astype(jnp.float32)
    receive(diagonal_copies())
    scale_more()

    complete(1)

    basis_high, basis_low = basis_parts[0], basis_parts[1]
    surface_high, surface_low = split(surface[...].reshape(nx * ny, nz))
    projected = (
        dot(surface_high, basis_high) + dot(surface_high, basis_low) + dot(surface_low, basis_high)
    )
    high, low = split(projected)
    looked = dot(onehot[...], high) + dot(onehot[...], low)
    turned = pltpu.roll(looked[lines:], LANES // 2, 1)
    spot = lax.broadcasted_iota(jnp.int32, (lines, LANES), 1)
    gradient = looked[:lines] + jnp.where(spot < LANES // 2, turned[lines:], turned[:lines])
    gradient = gradient * share
    for g in range(lines // rows):
        pieces[g] = gradient[g * rows : (g + 1) * rows]

    def group(gx, yz):
        return (gx * n_yz + yz) * per_owner // (rows * LANES)

    def give(c, gx, yz):
        remote(
            pieces.at[group(gx, yz)],
            arrived.at[me],
            (piece_sems.at[0], piece_sems.at[1]),
            (c, gx, yz),
        ).start()

    arrived[me] = pieces[group(xi, yi)]
    advance(len(rounds) - 1)
    if devices <= 64:
        turns = [(dc, dx, dy) for dc in range(n_cond) for dx in range(n_gx) for dy in range(n_yz)]
        ends = ((1, n_cond - 1), (1, n_gx - 1), (1, n_yz - 1))
        turns.sort(key=lambda t: -sum(d in e for d, e in zip(t, ends)))
        for dc, dx, dy in turns:
            if dc or dx or dy:
                give((ci + dc) % n_cond, (xi + dx) % n_gx, (yi + dy) % n_yz)
    else:

        def give_next(t, carry):
            flat = (me + t) % devices
            give(flat // (n_gx * n_yz), (flat // n_yz) % n_gx, flat % n_yz)
            return carry

        lax.fori_loop(1, devices, give_next, 0)

    for side, y in ((0, 0), (1, ny - 1)):
        for k in range(nvar):
            put_row(1, k, y, edges[2, side, k])
    for plans in copies(2):
        begin(plans)
    sweep(2, settle)
    complete(2)
    for stage in range(3):
        for plans in copies(stage):
            drain(plans)
    drain(corner_copies)
    drain(diagonal_copies())
    others = arrived.at[pl.ds(0, devices - 1)]
    for i in range(2):
        pltpu.make_async_copy(others, others, piece_sems.at[i]).wait()
    gradient_out[...] = jnp.sum(arrived[...], axis=0)


def write(smoothed, residual, gradient, smoothed_hbm, residual_hbm, gradient_hbm, sems):
    stores = [
        pltpu.make_async_copy(src, dst, sems.at[i])
        for i, (src, dst) in enumerate(
            ((smoothed, smoothed_hbm), (residual, residual_hbm), (gradient, gradient_hbm))
        )
    ]
    for copy in stores:
        copy.start()
    for copy in stores:
        copy.wait()


def local(
    adjoint,
    objective_gradient,
    diagonal,
    flux_blocks,
    flux_sensitivity,
    surface_mask,
    patch_band_slot,
    design_basis,
    condition_weights,
):
    sizes = tuple(lax.axis_size(axis) for axis in ("cond", "gx", "yz"))
    devices = sizes[0] * sizes[1] * sizes[2]
    _, nvar, nx, ny, nz = adjoint.shape
    per_owner = NDES // (sizes[1] * sizes[2])
    rows = max(1, per_owner // LANES)
    lines = NDES // LANES
    rounds = max(len(spans_of(sizes[1])), len(spans_of(sizes[2]))) + 2
    f32 = jnp.float32
    hbm = pl.BlockSpec(memory_space=pltpu.MemorySpace.HBM)
    vmem = pl.BlockSpec(memory_space=pltpu.MemorySpace.VMEM)
    depth = -(-3 * nvar * ny // (2 * LANES)) * 2 * LANES
    grant = 67043328 - 2**16 - 2 * adjoint.size * 4
    smoothed, residual, gradient = pl.pallas_call(
        functools.partial(kernel, sizes),
        out_shape=(
            pltpu.VMEM(adjoint.shape, f32),
            pltpu.VMEM(adjoint.shape, f32),
            pltpu.VMEM((rows, LANES), f32),
        ),
        in_specs=[hbm] * 9,
        out_specs=(vmem, vmem, vmem),
        scratch_shapes=[
            pltpu.VMEM((nvar + 1, nx, ny, nz), f32),
            pltpu.VMEM((nvar, nx, ny, nz), f32),
            pltpu.VMEM((nvar, nx, ny, nz), f32),
            pltpu.VMEM((nx, ny, nz), f32),
            pltpu.VMEM((5 * nvar * ny, depth), jnp.bfloat16),
            pltpu.VMEM((nx, depth, nz), jnp.bfloat16),
            pltpu.VMEM((nx, 5 * nvar * ny, nz), f32),
            pltpu.SMEM((nvar, nvar, 1, 6), f32),
            pltpu.VMEM((nvar, nx, ny, nz), jnp.bfloat16),
            pltpu.VMEM((nx, ny, nz), jnp.int32),
            pltpu.VMEM((nx, ny), jnp.int32),
            pltpu.VMEM(design_basis.shape, f32),
            pltpu.SMEM(condition_weights.shape, jnp.int32),
            pltpu.VMEM((nx, ny, nz), f32),
            pltpu.VMEM((4, 2, nvar + 1, nx, nz), f32),
            pltpu.VMEM((2, nvar, nx, nz), f32),
            pltpu.VMEM((2, nvar, ny, nz), f32),
            pltpu.VMEM((3, 2, nvar + 1, nx, nz), f32),
            pltpu.VMEM((3, 2, nvar + 1, ny, nz), f32),
            pltpu.VMEM((nvar, 8, nz), f32),
            pltpu.VMEM((2, nvar, nx, nz), f32),
            pltpu.VMEM((2, nvar, ny, nz), f32),
            pltpu.VMEM((2, nx, nz), f32),
            pltpu.VMEM((nvar, nx, ny, nz), f32),
            pltpu.VMEM((2, nvar, nx, nz), f32),
            pltpu.VMEM((2,) + design_basis.shape, jnp.bfloat16),
            pltpu.VMEM((3 * lines, nx * ny), jnp.bfloat16),
            pltpu.VMEM((NDES // (rows * LANES), rows, LANES), f32),
            pltpu.VMEM((devices, rows, LANES), f32),
            pltpu.SemaphoreType.DMA((2,)),
            pltpu.SemaphoreType.DMA((4,)),
            pltpu.SemaphoreType.DMA((3,)),
            pltpu.SemaphoreType.DMA((3, 2, 2)),
            pltpu.SemaphoreType.DMA((3, 2, 2)),
            pltpu.SemaphoreType.DMA((2, 4)),
            pltpu.SemaphoreType.DMA((2, 4)),
            pltpu.SemaphoreType.DMA((2,)),
            pltpu.SemaphoreType.REGULAR((rounds,)),
        ],
        compiler_params=pltpu.CompilerParams(
            collective_id=0, has_side_effects=True, vmem_limit_bytes=grant
        ),
    )(
        adjoint,
        objective_gradient,
        diagonal,
        jnp.transpose(flux_blocks, (2, 3, 0, 1)),
        flux_sensitivity,
        surface_mask,
        patch_band_slot,
        design_basis,
        condition_weights,
    )
    smoothed, residual, gradient = pl.pallas_call(
        write,
        out_shape=(
            jax.ShapeDtypeStruct(adjoint.shape, f32),
            jax.ShapeDtypeStruct(adjoint.shape, f32),
            jax.ShapeDtypeStruct((rows, LANES), f32),
        ),
        in_specs=[vmem] * 3,
        out_specs=(hbm, hbm, hbm),
        scratch_shapes=[pltpu.SemaphoreType.DMA((3,))],
        compiler_params=pltpu.CompilerParams(vmem_limit_bytes=2**20),
    )(smoothed, residual, gradient)
    flat = gradient.reshape(-1)
    if per_owner < flat.shape[0]:
        owner = lax.axis_index(("gx", "yz"))
        flat = lax.dynamic_slice_in_dim(flat, (owner * per_owner) % flat.shape[0], per_owner, 0)
    return smoothed, residual, flat


def solution(mesh):
    placed = (
        P("cond", None, "gx", "yz", None),
        P("cond", None, "gx", "yz", None),
        P("gx", "yz", None),
        P("cond", None, None, None),
        P("cond", None, "gx", "yz", None),
        P("gx", "yz", None),
        P("gx", "yz"),
        P(),
        P(),
    )
    return jax.shard_map(
        local,
        mesh=mesh,
        in_specs=placed,
        out_specs=(
            P("cond", None, "gx", "yz", None),
            P("cond", None, "gx", "yz", None),
            P(("gx", "yz")),
        ),
        check_vma=False,
    )
```

```python
import functools

import jax
import jax.numpy as jnp
from jax import lax
from jax.experimental import pallas as pl
from jax.experimental.pallas import tpu as pltpu
from jax.sharding import PartitionSpec as P

NDES = 4096
RELAX = 0.8
LANES = 128
PAD = 8
MESH = pl.DeviceIdType.MESH


def spans_of(count):
    reach, out = 1, []
    while reach < count - 1:
        out.append(reach)
        reach *= 2
    return out


def kernel(
    sizes,
    adjoint,
    source_hbm,
    diagonal_hbm,
    flux_hbm,
    sensitivity_hbm,
    mask_hbm,
    slots_hbm,
    basis_hbm,
    weights_hbm,
    smoothed_out,
    residual_out,
    arrived,
    first,
    second,
    source,
    step_of,
    bands,
    parts,
    products,
    flux,
    sensitivity,
    mask,
    slots,
    basis,
    weights,
    surface,
    edges,
    row_true,
    face_sent,
    row_halo,
    face_halo,
    corner,
    row_more,
    face_more,
    step_edge,
    weight,
    weight_edge,
    basis_parts,
    onehot,
    pieces,
    scalar_sems,
    local_sems,
    early_sems,
    row_sems,
    face_sems,
    corner_sems,
    diagonal_sems,
    piece_sems,
    round_sems,
):
    n_cond, n_gx, n_yz = sizes
    devices = n_cond * n_gx * n_yz
    nvar, nx, ny, nz = source.shape
    block = nvar * ny
    rows = pieces.shape[1]
    per_owner = NDES // (n_gx * n_yz)
    lines = NDES // LANES
    ci, xi, yi = lax.axis_index("cond"), lax.axis_index("gx"), lax.axis_index("yz")
    me = (ci * n_gx + xi) * n_yz + yi
    has_before_x, has_after_x = xi > 0, xi < n_gx - 1
    has_before_y, has_after_y = yi > 0, yi < n_yz - 1
    after_x, before_x = (ci, xi + 1, yi), (ci, xi - 1, yi)
    after_y, before_y = (ci, xi, yi + 1), (ci, xi, yi - 1)

    def signal(sem, target):
        pl.semaphore_signal(sem, inc=1, device_id=target, device_id_type=MESH)

    barrier = pltpu.get_barrier_semaphore()
    around = [
        (has_before_x, before_x),
        (has_after_x, after_x),
        (has_before_y, before_y),
        (has_after_y, after_y),
    ]
    diagonals = []
    for xs, there_x in ((-1, has_before_x), (1, has_after_x)):
        for ys, there_y in ((-1, has_before_y), (1, has_after_y)):
            diagonals.append((jnp.logical_and(there_x, there_y), (ci, xi + xs, yi + ys)))
    beside = n_cond - 1
    for there, target in around + diagonals:
        pl.when(there)(functools.partial(signal, barrier, target))
        beside = beside + there.astype(jnp.int32)
    for t in range(1, n_cond):
        signal(barrier, ((ci + t) % n_cond, xi, yi))

    scalar_loads = [
        pltpu.make_async_copy(flux_hbm, flux, scalar_sems.at[0]),
        pltpu.make_async_copy(weights_hbm, weights, scalar_sems.at[1]),
    ]
    adjoint_loads = [
        pltpu.make_async_copy(adjoint.at[0], first.at[pl.ds(0, nvar)], early_sems.at[0]),
        pltpu.make_async_copy(diagonal_hbm, first.at[nvar], early_sems.at[1]),
    ]
    source_loads = [pltpu.make_async_copy(source_hbm.at[0], source, early_sems.at[2])]

    late_loads = [
        pltpu.make_async_copy(src, dst, local_sems.at[i])
        for i, (src, dst) in enumerate(
            (
                (sensitivity_hbm.at[0], sensitivity),
                (mask_hbm, mask),
                (slots_hbm, slots),
                (basis_hbm, basis),
            )
        )
    ]
    for copy in scalar_loads + adjoint_loads + source_loads + late_loads:
        copy.start()

    def field(stage):
        return smoothed_out.at[0] if stage == 2 else (first, second)[stage]

    def clear_face(side):
        for stage in range(3):
            face_halo[stage, side] = jnp.zeros((nvar + 1, ny, nz), jnp.float32)
        face_halo[0, side, nvar] = jnp.ones((ny, nz), jnp.float32)

    def clear_row(side):
        for stage in range(3):
            row_halo[stage, side] = jnp.zeros((nvar + 1, nx, nz), jnp.float32)
        row_halo[0, side, nvar] = jnp.ones((nx, nz), jnp.float32)

    def clear_corner(i):
        corner[:, i : i + 1, :] = jnp.zeros((nvar, 1, nz), jnp.float32)

    corner[:, 4:, :] = jnp.zeros((nvar, 4, nz), jnp.float32)
    for i, (there, _) in enumerate(diagonals):
        pl.when(jnp.logical_not(there))(functools.partial(clear_corner, i))
    pl.when(xi == 0)(functools.partial(clear_face, 0))
    pl.when(xi == n_gx - 1)(functools.partial(clear_face, 1))
    pl.when(yi == 0)(functools.partial(clear_row, 0))
    pl.when(yi == n_yz - 1)(functools.partial(clear_row, 1))
    depth = parts.shape[1]
    if depth > 3 * block:
        for x in range(nx):
            parts[x, 3 * block :] = jnp.zeros((depth - 3 * block, nz), jnp.bfloat16)

    def remote(src, dst, sems, target):
        return pltpu.make_async_remote_copy(
            src_ref=src,
            dst_ref=dst,
            send_sem=sems[0],
            recv_sem=sems[1],
            device_id=target,
            device_id_type=MESH,
        )

    def copies(stage):
        sent = pl.ds(0, nvar)

        def face(side, x):
            return face_sent.at[side] if stage == 1 else field(stage).at[sent, x]

        def sems(ref, way):
            return ref.at[stage, 0, way], ref.at[stage, 1, way]

        def into(ref, side):
            return ref.at[stage, side, sent]

        up_x = remote(face(1, nx - 1), into(face_halo, 0), sems(face_sems, 0), after_x)
        down_x = remote(face(0, 0), into(face_halo, 1), sems(face_sems, 1), before_x)
        up_y = remote(edges.at[stage, 1, sent], into(row_halo, 0), sems(row_sems, 0), after_y)
        down_y = remote(edges.at[stage, 0, sent], into(row_halo, 1), sems(row_sems, 1), before_y)
        return (
            [(has_after_x, has_before_x, up_x), (has_before_x, has_after_x, down_x)],
            [(has_after_y, has_before_y, up_y), (has_before_y, has_after_y, down_y)],
        )

    def diagonal_copies():
        def sems(way):
            return diagonal_sems.at[0, way], diagonal_sems.at[1, way]

        up_x = remote(first.at[nvar, nx - 1], face_halo.at[0, 0, nvar], sems(0), after_x)
        down_x = remote(first.at[nvar, 0], face_halo.at[0, 1, nvar], sems(1), before_x)
        up_y = remote(edges.at[0, 1, nvar], row_halo.at[0, 0, nvar], sems(2), after_y)
        down_y = remote(edges.at[0, 0, nvar], row_halo.at[0, 1, nvar], sems(3), before_y)
        return [
            (has_after_x, has_before_x, up_x),
            (has_before_x, has_after_x, down_x),
            (has_after_y, has_before_y, up_y),
            (has_before_y, has_after_y, down_y),
        ]

    corner_copies = []
    for i, (there, target) in enumerate(diagonals):
        x, side = (0, nx - 1)[i // 2], i % 2
        copy = remote(
            edges.at[0, side, pl.ds(0, nvar), pl.ds(x, 1), :],
            corner.at[:, pl.ds(3 - i, 1), :],
            (corner_sems.at[0, i], corner_sems.at[1, i]),
            target,
        )
        corner_copies.append((there, diagonals[3 - i][0], copy))

    def begin(plans):
        for go, _, copy in plans:
            pl.when(go)(copy.start)

    def receive(plans):
        for _, come, copy in plans:
            pl.when(come)(copy.wait_recv)

    def drain(plans):
        for go, _, copy in plans:
            pl.when(go)(copy.wait_send)

    def line_round(distances):
        targets = []
        for axis, distance in distances:
            here, count = (xi, n_gx) if axis == "gx" else (yi, n_yz)
            for sign in (1, -1):
                there = here + sign * distance
                target = (ci, there, yi) if axis == "gx" else (ci, xi, there)
                targets.append((jnp.logical_and(there >= 0, there < count), target))
        return targets

    gx_spans, yz_spans = spans_of(n_gx), spans_of(n_yz)
    rounds = []
    for i in range(max(len(gx_spans), len(yz_spans))):
        distances = [("gx", d) for d in gx_spans[i : i + 1]] + [("yz", d) for d in yz_spans[i : i + 1]]
        rounds.append(line_round(distances))
    always = ci >= 0
    rounds.append([(always, (ci, (xi + t) % n_gx, yi)) for t in range(1, n_gx)])
    rounds.append([(always, ((ci + t) % n_cond, xi, yi)) for t in range(1, n_cond)])

    def tell(i):
        for there, target in rounds[i]:
            pl.when(there)(functools.partial(signal, round_sems.at[i], target))

    def hear(i):
        count = 0
        for there, _ in rounds[i]:
            count = count + there.astype(jnp.int32)
        pl.semaphore_wait(round_sems.at[i], count)

    def advance(i):
        hear(i)
        if i + 1 < len(rounds):
            tell(i + 1)

    def keep_edges(kept, k, x, value):
        kept[0, k, x : x + 1, :] = value[0:1]
        kept[1, k, x : x + 1, :] = value[ny - 1 : ny]

    def rows_of(stage):
        return row_true if stage == 1 else edges.at[stage]

    def split(value):
        high = value.astype(jnp.bfloat16)
        return high, (value - high.astype(jnp.float32)).astype(jnp.bfloat16)

    column = lax.broadcasted_iota(jnp.int32, (ny, depth), 1)
    row = lax.broadcasted_iota(jnp.int32, (ny, depth), 0)
    part = column // block
    pair = column - part * block
    from_var = pair // ny
    offset = pair - from_var * ny - row

    for copy in scalar_loads:
        copy.wait()

    def spread(k, d):
        total = jnp.zeros((ny, depth), jnp.float32)
        for e in range(nvar):
            total = jnp.where(from_var == e, flux[e, k, 0, d], total)
        upper = total.astype(jnp.bfloat16).astype(jnp.float32)
        lower = (total - upper).astype(jnp.bfloat16).astype(jnp.float32)
        return jnp.where(part < 2, upper, jnp.where(part == 2, lower, 0.0))

    for k in range(nvar):
        own = jnp.where(offset == 1, spread(k, 2), jnp.where(offset == -1, spread(k, 3), 0.0))
        bands[k * ny : (k + 1) * ny, :] = own.astype(jnp.bfloat16)
        for g, d in ((1, 0), (2, 1), (3, 4), (4, 5)):
            other = jnp.where(offset == 0, spread(k, d), 0.0)
            at = g * block + k * ny
            bands[at : at + ny, :] = other.astype(jnp.bfloat16)

    pl.semaphore_wait(barrier, beside)
    tell(0)
    for copy in adjoint_loads:
        copy.wait()
    for x in range(nx):
        for k in range(nvar + 1):
            keep_edges(edges.at[0], k, x, first[k, x])
    for plans in copies(0):
        begin(plans)
    begin(corner_copies)
    begin(diagonal_copies())

    dot = functools.partial(jnp.dot, preferred_element_type=jnp.float32)
    lane = lax.broadcasted_iota(jnp.int32, (ny, LANES), 1)
    spans = [slice(h * LANES, (h + 1) * LANES) for h in range(nz // LANES)]

    def multiply(stage, x):
        for e in range(nvar):
            high, low = split(field(stage)[e, x])
            for p, value in enumerate((high, low, high)):
                at = p * block + e * ny
                parts[x, at : at + ny, :] = value
        products[x] = dot(bands[...], parts[x])

    def gathered(x, k):
        def product(plane, g):
            at = g * block + k * ny
            return products[plane, at : at + ny, :]

        acc = source[k, x] + product(x, 0)
        if x + 1 < nx:
            acc = acc + product(x + 1, 1)
        if x > 0:
            acc = acc + product(x - 1, 2)
        ahead = [pltpu.roll(product(x, 3)[:, c], LANES - 1, 1) for c in spans] + [0.0]
        behind = [0.0] + [pltpu.roll(product(x, 4)[:, c], 1, 1) for c in spans]
        shifted = [
            jnp.where(lane == LANES - 1, ahead[h + 1], ahead[h])
            + jnp.where(lane == 0, behind[h], behind[h + 1])
            for h in range(len(spans))
        ]
        return acc + jnp.concatenate(shifted, axis=1)

    def relax(stage, x):
        if stage == 0:
            step = RELAX / first[nvar, x]
            step_of[x] = step
            step_edge[0, x : x + 1, :] = step[0:1]
            step_edge[1, x : x + 1, :] = step[ny - 1 : ny]
        else:
            step = step_of[x]
        total = None
        for k in range(nvar):
            value = (1.0 - RELAX) * field(stage)[k, x] + step * gathered(x, k)
            field(stage + 1)[k, x] = value
            keep_edges(edges.at[stage + 1], k, x, value)
            if stage == 0:
                keep_edges(row_true, k, x, value)
                for side, plane in ((0, 0), (1, nx - 1)):
                    if x == plane:
                        face_sent[side, k] = value
            if stage == 1:
                term = value * weight[k, x]
                total = term if k == 0 else total + term
        if stage == 1:
            surface[x] = total

    def settle(stage, x):
        for k in range(nvar):
            value = gathered(x, k) - first[nvar, x] * field(2)[k, x]
            residual_out[0, k, x] = value
            keep_edges(edges.at[3], k, x, value)

    def sweep(stage, finish):
        multiply(stage, 0)
        for x in range(nx):
            if x + 1 < nx:
                multiply(stage, x + 1)
            finish(stage, x)

    def brought(cells, d):
        out = []
        for k in range(nvar):
            total = flux[0, k, 0, d] * cells[0]
            for e in range(1, nvar):
                total = total + flux[e, k, 0, d] * cells[e]
            out.append(total)
        return out

    def halo_of(halo, more, stage, side):
        cells = [halo[stage, side, e] for e in range(nvar)]
        return [c + more[side, e] for e, c in enumerate(cells)] if stage == 1 else cells

    def begin_own():
        for side, d in ((0, 2), (1, 3)):
            mine = brought([edges[0, side, e] for e in range(nvar)], d)
            for k in range(nvar):
                row_more[side, k] = mine[k]
        for side, x, d in ((0, 0, 0), (1, nx - 1, 1)):
            mine = brought([first[e, x] for e in range(nvar)], d)
            for k in range(nvar):
                face_more[side, k] = mine[k]

    def add_corners():
        spot = lax.broadcasted_iota(jnp.int32, (8, nz), 0)
        lines_of = [corner[e] for e in range(nvar)]
        at_row = lax.broadcasted_iota(jnp.int32, (nx, nz), 0)
        at_face = lax.broadcasted_iota(jnp.int32, (ny, nz), 0)
        for k in range(nvar):
            along = []
            for near, ds in ((spot < 2, (1, 0)), (spot % 2 == 0, (3, 2))):
                total = None
                for e in range(nvar):
                    scale = jnp.where(near, flux[e, k, 0, ds[0]], flux[e, k, 0, ds[1]])
                    term = scale * lines_of[e]
                    total = term if e == 0 else total + term
                along.append(total)
            for side in range(2):
                ends = along[0][side : side + 1], along[0][2 + side : 3 + side]
                extra = jnp.where(at_row == 0, ends[0], jnp.where(at_row == nx - 1, ends[1], 0.0))
                row_more[side, k] = row_more[side, k] + extra
                ends = along[1][2 * side : 2 * side + 1], along[1][2 * side + 1 : 2 * side + 2]
                extra = jnp.where(at_face == 0, ends[0], jnp.where(at_face == ny - 1, ends[1], 0.0))
                face_more[side, k] = face_more[side, k] + extra

    def scale_more():
        for side, there in ((0, has_before_y), (1, has_after_y)):
            step = jnp.where(there, RELAX / row_halo[0, side, nvar], 0.0)
            for k in range(nvar):
                row_more[side, k] = step * row_more[side, k]
        for side, there in ((0, has_before_x), (1, has_after_x)):
            step = jnp.where(there, RELAX / face_halo[0, side, nvar], 0.0)
            for k in range(nvar):
                face_more[side, k] = step * face_more[side, k]

    def add_faces(stage):
        for side, x, d in ((0, 0, 1), (1, nx - 1, 0)):
            more = brought(halo_of(face_halo, face_more, stage, side), d)
            total = None
            for k in range(nvar):
                if stage == 2:
                    value = residual_out[0, k, x] + more[k]
                    residual_out[0, k, x] = value
                else:
                    part = step_of[x] * more[k]
                    value = field(stage + 1)[k, x] + part
                    field(stage + 1)[k, x] = value
                    if stage == 1:
                        term = part * weight[k, x]
                        total = term if k == 0 else total + term
                keep_edges(rows_of(stage + 1), k, x, value)
            if stage == 1:
                surface[x] = surface[x] + total

    def put_row(stage, k, y, value):
        for x in range(nx):
            if stage == 2:
                residual_out[0, k, x, y : y + 1, :] = value[x : x + 1]
            else:
                field(stage + 1)[k, x, y : y + 1, :] = value[x : x + 1]

    def add_rows(stage):
        for side, y, d in ((0, 0, 3), (1, ny - 1, 2)):
            more = brought(halo_of(row_halo, row_more, stage, side), d)
            total = None
            for k in range(nvar):
                part = more[k] if stage == 2 else step_edge[side] * more[k]
                value = rows_of(stage + 1)[side, k] + part
                if stage == 1:
                    edges[2, side, k] = value
                if stage == 1:
                    term = part * weight_edge[side, k]
                    total = term if k == 0 else total + term
                if stage != 1:
                    put_row(stage, k, y, value)
            if stage == 1:
                for x in range(nx):
                    surface[x, y : y + 1, :] = surface[x, y : y + 1, :] + total[x : x + 1]

    def complete(stage):
        faces, ranks = copies(stage)
        receive(faces)
        add_faces(stage)
        receive(ranks)
        add_rows(stage)

    for copy in source_loads:
        copy.wait()
    advance(0)
    sweep(0, relax)
    for plans in copies(1):
        begin(plans)
    begin_own()
    for copy in late_loads:
        copy.wait()
    for x in range(nx):
        cover = mask[x].astype(jnp.float32)
        for k in range(nvar):
            value = sensitivity[k, x].astype(jnp.float32) * cover
            weight[k, x] = value
            keep_edges(weight_edge, k, x, value)
    basis_parts[0], basis_parts[1] = split(basis[...])
    line = lax.broadcasted_iota(jnp.int32, (lines, nx * ny), 0)
    spots = jnp.concatenate([slots[x : x + 1, :] for x in range(nx)], axis=1)
    wanted = jnp.concatenate([2 * line, 2 * line + 1, 2 * line - 1], axis=0)
    onehot[...] = (wanted == spots).astype(jnp.float32).astype(jnp.bfloat16)
    for i in range(1, len(rounds) - 2):
        advance(i)
    complete(0)
    advance(len(rounds) - 2)
    receive(corner_copies)
    add_corners()
    sweep(1, relax)
    weight_sum = weights[0]
    for c in range(1, n_cond):
        weight_sum = weight_sum + weights[c]
    share = jnp.full((1, LANES), weights[ci], jnp.int32).astype(jnp.float32) / jnp.full(
        (1, LANES), weight_sum, jnp.int32
    ).astype(jnp.float32)
    receive(diagonal_copies())
    scale_more()

    complete(1)

    basis_high, basis_low = basis_parts[0], basis_parts[1]
    surface_high, surface_low = split(surface[...].reshape(nx * ny, nz))
    projected = (
        dot(surface_high, basis_high) + dot(surface_high, basis_low) + dot(surface_low, basis_high)
    )
    high, low = split(projected)
    looked = dot(onehot[...], high) + dot(onehot[...], low)
    turned = pltpu.roll(looked[lines:], LANES // 2, 1)
    spot = lax.broadcasted_iota(jnp.int32, (lines, LANES), 1)
    gradient = looked[:lines] + jnp.where(spot < LANES // 2, turned[lines:], turned[:lines])
    gradient = gradient * share
    for g in range(lines // rows):
        pieces[g] = gradient[g * rows : (g + 1) * rows]

    def group(gx, yz):
        return (gx * n_yz + yz) * per_owner // (rows * LANES)

    def give(c, gx, yz):
        remote(
            pieces.at[group(gx, yz)],
            arrived.at[me],
            (piece_sems.at[0], piece_sems.at[1]),
            (c, gx, yz),
        ).start()

    arrived[me] = pieces[group(xi, yi)]
    advance(len(rounds) - 1)
    if devices <= 64:
        turns = [(dc, dx, dy) for dc in range(n_cond) for dx in range(n_gx) for dy in range(n_yz)]
        ends = ((1, n_cond - 1), (1, n_gx - 1), (1, n_yz - 1))
        turns.sort(key=lambda t: -sum(d in e for d, e in zip(t, ends)))
        for dc, dx, dy in turns:
            if dc or dx or dy:
                give((ci + dc) % n_cond, (xi + dx) % n_gx, (yi + dy) % n_yz)
    else:

        def give_next(t, carry):
            flat = (me + t) % devices
            give(flat // (n_gx * n_yz), (flat // n_yz) % n_gx, flat % n_yz)
            return carry

        lax.fori_loop(1, devices, give_next, 0)

    for side, y in ((0, 0), (1, ny - 1)):
        for k in range(nvar):
            put_row(1, k, y, edges[2, side, k])
    for plans in copies(2):
        begin(plans)
    sweep(2, settle)
    complete(2)
    for stage in range(3):
        for plans in copies(stage):
            drain(plans)
    drain(corner_copies)
    drain(diagonal_copies())
    others = arrived.at[pl.ds(0, devices - 1)]
    for i in range(2):
        pltpu.make_async_copy(others, others, piece_sems.at[i]).wait()


def write(smoothed, residual, arrived, smoothed_hbm, residual_hbm, gradient_hbm, gradient, sems):
    stores = [
        pltpu.make_async_copy(src, dst, sems.at[i])
        for i, (src, dst) in enumerate(
            ((smoothed, smoothed_hbm), (residual, residual_hbm), (gradient, gradient_hbm))
        )
    ]
    for copy in stores[:2]:
        copy.start()
    gradient[...] = jnp.sum(arrived[...], axis=0)
    stores[2].start()
    for copy in stores:
        copy.wait()


def local(
    adjoint,
    objective_gradient,
    diagonal,
    flux_blocks,
    flux_sensitivity,
    surface_mask,
    patch_band_slot,
    design_basis,
    condition_weights,
):
    sizes = tuple(lax.axis_size(axis) for axis in ("cond", "gx", "yz"))
    devices = sizes[0] * sizes[1] * sizes[2]
    _, nvar, nx, ny, nz = adjoint.shape
    per_owner = NDES // (sizes[1] * sizes[2])
    rows = max(1, per_owner // LANES)
    lines = NDES // LANES
    rounds = max(len(spans_of(sizes[1])), len(spans_of(sizes[2]))) + 2
    f32 = jnp.float32
    hbm = pl.BlockSpec(memory_space=pltpu.MemorySpace.HBM)
    vmem = pl.BlockSpec(memory_space=pltpu.MemorySpace.VMEM)
    depth = -(-3 * nvar * ny // (2 * LANES)) * 2 * LANES
    grant = 67043328 - 2**16 - 2 * adjoint.size * 4 - 2**12 * devices
    smoothed, residual, arrived = pl.pallas_call(
        functools.partial(kernel, sizes),
        out_shape=(
            pltpu.VMEM(adjoint.shape, f32),
            pltpu.VMEM(adjoint.shape, f32),
            pltpu.VMEM((devices, rows, LANES), f32),
        ),
        in_specs=[hbm] * 9,
        out_specs=(vmem, vmem, vmem),
        scratch_shapes=[
            pltpu.VMEM((nvar + 1, nx, ny, nz), f32),
            pltpu.VMEM((nvar, nx, ny, nz), f32),
            pltpu.VMEM((nvar, nx, ny, nz), f32),
            pltpu.VMEM((nx, ny, nz), f32),
            pltpu.VMEM((5 * nvar * ny, depth), jnp.bfloat16),
            pltpu.VMEM((nx, depth, nz), jnp.bfloat16),
            pltpu.VMEM((nx, 5 * nvar * ny, nz), f32),
            pltpu.SMEM((nvar, nvar, 1, 6), f32),
            pltpu.VMEM((nvar, nx, ny, nz), jnp.bfloat16),
            pltpu.VMEM((nx, ny, nz), jnp.int32),
            pltpu.VMEM((nx, ny), jnp.int32),
            pltpu.VMEM(design_basis.shape, f32),
            pltpu.SMEM(condition_weights.shape, jnp.int32),
            pltpu.VMEM((nx, ny, nz), f32),
            pltpu.VMEM((4, 2, nvar + 1, nx, nz), f32),
            pltpu.VMEM((2, nvar, nx, nz), f32),
            pltpu.VMEM((2, nvar, ny, nz), f32),
            pltpu.VMEM((3, 2, nvar + 1, nx, nz), f32),
            pltpu.VMEM((3, 2, nvar + 1, ny, nz), f32),
            pltpu.VMEM((nvar, 8, nz), f32),
            pltpu.VMEM((2, nvar, nx, nz), f32),
            pltpu.VMEM((2, nvar, ny, nz), f32),
            pltpu.VMEM((2, nx, nz), f32),
            pltpu.VMEM((nvar, nx, ny, nz), f32),
            pltpu.VMEM((2, nvar, nx, nz), f32),
            pltpu.VMEM((2,) + design_basis.shape, jnp.bfloat16),
            pltpu.VMEM((3 * lines, nx * ny), jnp.bfloat16),
            pltpu.VMEM((NDES // (rows * LANES), rows, LANES), f32),
            pltpu.SemaphoreType.DMA((2,)),
            pltpu.SemaphoreType.DMA((4,)),
            pltpu.SemaphoreType.DMA((3,)),
            pltpu.SemaphoreType.DMA((3, 2, 2)),
            pltpu.SemaphoreType.DMA((3, 2, 2)),
            pltpu.SemaphoreType.DMA((2, 4)),
            pltpu.SemaphoreType.DMA((2, 4)),
            pltpu.SemaphoreType.DMA((2,)),
            pltpu.SemaphoreType.REGULAR((rounds,)),
        ],
        compiler_params=pltpu.CompilerParams(
            collective_id=0, has_side_effects=True, vmem_limit_bytes=grant
        ),
    )(
        adjoint,
        objective_gradient,
        diagonal,
        jnp.transpose(flux_blocks, (2, 3, 0, 1)),
        flux_sensitivity,
        surface_mask,
        patch_band_slot,
        design_basis,
        condition_weights,
    )
    smoothed, residual, gradient = pl.pallas_call(
        write,
        out_shape=(
            jax.ShapeDtypeStruct(adjoint.shape, f32),
            jax.ShapeDtypeStruct(adjoint.shape, f32),
            jax.ShapeDtypeStruct((rows, LANES), f32),
        ),
        in_specs=[vmem] * 3,
        out_specs=(hbm, hbm, hbm),
        scratch_shapes=[pltpu.VMEM((rows, LANES), f32), pltpu.SemaphoreType.DMA((3,))],
        compiler_params=pltpu.CompilerParams(vmem_limit_bytes=2**20),
    )(smoothed, residual, arrived)
    flat = gradient.reshape(-1)
    if per_owner < flat.shape[0]:
        owner = lax.axis_index(("gx", "yz"))
        flat = lax.dynamic_slice_in_dim(flat, (owner * per_owner) % flat.shape[0], per_owner, 0)
    return smoothed, residual, flat


def solution(mesh):
    placed = (
        P("cond", None, "gx", "yz", None),
        P("cond", None, "gx", "yz", None),
        P("gx", "yz", None),
        P("cond", None, None, None),
        P("cond", None, "gx", "yz", None),
        P("gx", "yz", None),
        P("gx", "yz"),
        P(),
        P(),
    )
    return jax.shard_map(
        local,
        mesh=mesh,
        in_specs=placed,
        out_specs=(
            P("cond", None, "gx", "yz", None),
            P("cond", None, "gx", "yz", None),
            P(("gx", "yz")),
        ),
        check_vma=False,
    )
```

```python
import functools

import jax
import jax.numpy as jnp
from jax import lax
from jax.experimental import pallas as pl
from jax.experimental.pallas import tpu as pltpu
from jax.sharding import PartitionSpec as P

NDES = 4096
RELAX = 0.8
LANES = 128
PAD = 8
MESH = pl.DeviceIdType.MESH


def spans_of(count):
    reach, out = 1, []
    while reach < count - 1:
        out.append(reach)
        reach *= 2
    return out


def kernel(
    sizes,
    adjoint,
    source_hbm,
    diagonal_hbm,
    flux_hbm,
    sensitivity_hbm,
    mask_hbm,
    slots_hbm,
    basis_hbm,
    weights_hbm,
    smoothed_out,
    residual_out,
    arrived,
    first,
    second,
    source,
    step_of,
    bands,
    parts,
    products,
    flux,
    sensitivity,
    mask,
    slots,
    basis,
    weights,
    surface,
    edges,
    row_true,
    face_sent,
    row_halo,
    face_halo,
    corner,
    row_more,
    face_more,
    step_edge,
    weight,
    weight_edge,
    basis_parts,
    onehot,
    pieces,
    scalar_sems,
    local_sems,
    early_sems,
    row_sems,
    face_sems,
    corner_sems,
    diagonal_sems,
    piece_sems,
    round_sems,
):
    n_cond, n_gx, n_yz = sizes
    devices = n_cond * n_gx * n_yz
    nvar, nx, ny, nz = source.shape
    block = nvar * ny
    rows = pieces.shape[1]
    per_owner = NDES // (n_gx * n_yz)
    lines = NDES // LANES
    ci, xi, yi = lax.axis_index("cond"), lax.axis_index("gx"), lax.axis_index("yz")
    me = (ci * n_gx + xi) * n_yz + yi
    has_before_x, has_after_x = xi > 0, xi < n_gx - 1
    has_before_y, has_after_y = yi > 0, yi < n_yz - 1
    after_x, before_x = (ci, xi + 1, yi), (ci, xi - 1, yi)
    after_y, before_y = (ci, xi, yi + 1), (ci, xi, yi - 1)

    def signal(sem, target):
        pl.semaphore_signal(sem, inc=1, device_id=target, device_id_type=MESH)

    barrier = pltpu.get_barrier_semaphore()
    around = [
        (has_before_x, before_x),
        (has_after_x, after_x),
        (has_before_y, before_y),
        (has_after_y, after_y),
    ]
    diagonals = []
    for xs, there_x in ((-1, has_before_x), (1, has_after_x)):
        for ys, there_y in ((-1, has_before_y), (1, has_after_y)):
            diagonals.append((jnp.logical_and(there_x, there_y), (ci, xi + xs, yi + ys)))
    beside = n_cond - 1
    for there, target in around + diagonals:
        pl.when(there)(functools.partial(signal, barrier, target))
        beside = beside + there.astype(jnp.int32)
    for t in range(1, n_cond):
        signal(barrier, ((ci + t) % n_cond, xi, yi))

    scalar_loads = [
        pltpu.make_async_copy(flux_hbm, flux, scalar_sems.at[0]),
        pltpu.make_async_copy(weights_hbm, weights, scalar_sems.at[1]),
    ]
    adjoint_loads = [
        pltpu.make_async_copy(adjoint.at[0], first.at[pl.ds(0, nvar)], early_sems.at[0]),
        pltpu.make_async_copy(diagonal_hbm, first.at[nvar], early_sems.at[1]),
    ]
    source_loads = [pltpu.make_async_copy(source_hbm.at[0], source, early_sems.at[2])]

    late_loads = [
        pltpu.make_async_copy(src, dst, local_sems.at[i])
        for i, (src, dst) in enumerate(
            (
                (sensitivity_hbm.at[0], sensitivity),
                (mask_hbm, mask),
                (slots_hbm, slots),
                (basis_hbm, basis),
            )
        )
    ]
    for copy in scalar_loads + adjoint_loads + source_loads:
        copy.start()

    def field(stage):
        return smoothed_out.at[0] if stage == 2 else (first, second)[stage]

    def clear_face(side):
        for stage in range(3):
            face_halo[stage, side] = jnp.zeros((nvar + 1, ny, nz), jnp.float32)
        face_halo[0, side, nvar] = jnp.ones((ny, nz), jnp.float32)

    def clear_row(side):
        for stage in range(3):
            row_halo[stage, side] = jnp.zeros((nvar + 1, nx, nz), jnp.float32)
        row_halo[0, side, nvar] = jnp.ones((nx, nz), jnp.float32)

    def clear_corner(i):
        corner[:, i : i + 1, :] = jnp.zeros((nvar, 1, nz), jnp.float32)

    corner[:, 4:, :] = jnp.zeros((nvar, 4, nz), jnp.float32)
    for i, (there, _) in enumerate(diagonals):
        pl.when(jnp.logical_not(there))(functools.partial(clear_corner, i))
    pl.when(xi == 0)(functools.partial(clear_face, 0))
    pl.when(xi == n_gx - 1)(functools.partial(clear_face, 1))
    pl.when(yi == 0)(functools.partial(clear_row, 0))
    pl.when(yi == n_yz - 1)(functools.partial(clear_row, 1))
    depth = parts.shape[1]
    if depth > 3 * block:
        for x in range(nx):
            parts[x, 3 * block :] = jnp.zeros((depth - 3 * block, nz), jnp.bfloat16)

    def remote(src, dst, sems, target):
        return pltpu.make_async_remote_copy(
            src_ref=src,
            dst_ref=dst,
            send_sem=sems[0],
            recv_sem=sems[1],
            device_id=target,
            device_id_type=MESH,
        )

    def copies(stage):
        sent = pl.ds(0, nvar)

        def face(side, x):
            return face_sent.at[side] if stage == 1 else field(stage).at[sent, x]

        def sems(ref, way):
            return ref.at[stage, 0, way], ref.at[stage, 1, way]

        def into(ref, side):
            return ref.at[stage, side, sent]

        up_x = remote(face(1, nx - 1), into(face_halo, 0), sems(face_sems, 0), after_x)
        down_x = remote(face(0, 0), into(face_halo, 1), sems(face_sems, 1), before_x)
        up_y = remote(edges.at[stage, 1, sent], into(row_halo, 0), sems(row_sems, 0), after_y)
        down_y = remote(edges.at[stage, 0, sent], into(row_halo, 1), sems(row_sems, 1), before_y)
        return (
            [(has_after_x, has_before_x, up_x), (has_before_x, has_after_x, down_x)],
            [(has_after_y, has_before_y, up_y), (has_before_y, has_after_y, down_y)],
        )

    def diagonal_copies():
        def sems(way):
            return diagonal_sems.at[0, way], diagonal_sems.at[1, way]

        up_x = remote(first.at[nvar, nx - 1], face_halo.at[0, 0, nvar], sems(0), after_x)
        down_x = remote(first.at[nvar, 0], face_halo.at[0, 1, nvar], sems(1), before_x)
        up_y = remote(edges.at[0, 1, nvar], row_halo.at[0, 0, nvar], sems(2), after_y)
        down_y = remote(edges.at[0, 0, nvar], row_halo.at[0, 1, nvar], sems(3), before_y)
        return [
            (has_after_x, has_before_x, up_x),
            (has_before_x, has_after_x, down_x),
            (has_after_y, has_before_y, up_y),
            (has_before_y, has_after_y, down_y),
        ]

    corner_copies = []
    for i, (there, target) in enumerate(diagonals):
        x, side = (0, nx - 1)[i // 2], i % 2
        copy = remote(
            edges.at[0, side, pl.ds(0, nvar), pl.ds(x, 1), :],
            corner.at[:, pl.ds(3 - i, 1), :],
            (corner_sems.at[0, i], corner_sems.at[1, i]),
            target,
        )
        corner_copies.append((there, diagonals[3 - i][0], copy))

    def begin(plans):
        for go, _, copy in plans:
            pl.when(go)(copy.start)

    def receive(plans):
        for _, come, copy in plans:
            pl.when(come)(copy.wait_recv)

    def drain(plans):
        for go, _, copy in plans:
            pl.when(go)(copy.wait_send)

    def line_round(distances):
        targets = []
        for axis, distance in distances:
            here, count = (xi, n_gx) if axis == "gx" else (yi, n_yz)
            for sign in (1, -1):
                there = here + sign * distance
                target = (ci, there, yi) if axis == "gx" else (ci, xi, there)
                targets.append((jnp.logical_and(there >= 0, there < count), target))
        return targets

    gx_spans, yz_spans = spans_of(n_gx), spans_of(n_yz)
    rounds = []
    for i in range(max(len(gx_spans), len(yz_spans))):
        distances = [("gx", d) for d in gx_spans[i : i + 1]] + [("yz", d) for d in yz_spans[i : i + 1]]
        rounds.append(line_round(distances))
    always = ci >= 0
    rounds.append([(always, (ci, (xi + t) % n_gx, yi)) for t in range(1, n_gx)])
    rounds.append([(always, ((ci + t) % n_cond, xi, yi)) for t in range(1, n_cond)])

    def tell(i):
        for there, target in rounds[i]:
            pl.when(there)(functools.partial(signal, round_sems.at[i], target))

    def hear(i):
        count = 0
        for there, _ in rounds[i]:
            count = count + there.astype(jnp.int32)
        pl.semaphore_wait(round_sems.at[i], count)

    def advance(i):
        hear(i)
        if i + 1 < len(rounds):
            tell(i + 1)

    def keep_edges(kept, k, x, value):
        kept[0, k, x : x + 1, :] = value[0:1]
        kept[1, k, x : x + 1, :] = value[ny - 1 : ny]

    def rows_of(stage):
        return row_true if stage == 1 else edges.at[stage]

    def split(value):
        high = value.astype(jnp.bfloat16)
        return high, (value - high.astype(jnp.float32)).astype(jnp.bfloat16)

    column = lax.broadcasted_iota(jnp.int32, (ny, depth), 1)
    row = lax.broadcasted_iota(jnp.int32, (ny, depth), 0)
    part = column // block
    pair = column - part * block
    from_var = pair // ny
    offset = pair - from_var * ny - row

    for copy in scalar_loads:
        copy.wait()

    def spread(k, d):
        total = jnp.zeros((ny, depth), jnp.float32)
        for e in range(nvar):
            total = jnp.where(from_var == e, flux[e, k, 0, d], total)
        upper = total.astype(jnp.bfloat16).astype(jnp.float32)
        lower = (total - upper).astype(jnp.bfloat16).astype(jnp.float32)
        return jnp.where(part < 2, upper, jnp.where(part == 2, lower, 0.0))

    for k in range(nvar):
        own = jnp.where(offset == 1, spread(k, 2), jnp.where(offset == -1, spread(k, 3), 0.0))
        bands[k * ny : (k + 1) * ny, :] = own.astype(jnp.bfloat16)
        for g, d in ((1, 0), (2, 1), (3, 4), (4, 5)):
            other = jnp.where(offset == 0, spread(k, d), 0.0)
            at = g * block + k * ny
            bands[at : at + ny, :] = other.astype(jnp.bfloat16)

    pl.semaphore_wait(barrier, beside)
    tell(0)
    for copy in adjoint_loads:
        copy.wait()
    for x in range(nx):
        for k in range(nvar + 1):
            keep_edges(edges.at[0], k, x, first[k, x])
    for plans in copies(0):
        begin(plans)
    begin(corner_copies)
    begin(diagonal_copies())
    for copy in late_loads:
        copy.start()

    dot = functools.partial(jnp.dot, preferred_element_type=jnp.float32)
    lane = lax.broadcasted_iota(jnp.int32, (ny, LANES), 1)
    spans = [slice(h * LANES, (h + 1) * LANES) for h in range(nz // LANES)]

    def multiply(stage, x):
        for e in range(nvar):
            high, low = split(field(stage)[e, x])
            for p, value in enumerate((high, low, high)):
                at = p * block + e * ny
                parts[x, at : at + ny, :] = value
        products[x] = dot(bands[...], parts[x])

    def gathered(x, k):
        def product(plane, g):
            at = g * block + k * ny
            return products[plane, at : at + ny, :]

        acc = source[k, x] + product(x, 0)
        if x + 1 < nx:
            acc = acc + product(x + 1, 1)
        if x > 0:
            acc = acc + product(x - 1, 2)
        ahead = [pltpu.roll(product(x, 3)[:, c], LANES - 1, 1) for c in spans] + [0.0]
        behind = [0.0] + [pltpu.roll(product(x, 4)[:, c], 1, 1) for c in spans]
        shifted = [
            jnp.where(lane == LANES - 1, ahead[h + 1], ahead[h])
            + jnp.where(lane == 0, behind[h], behind[h + 1])
            for h in range(len(spans))
        ]
        return acc + jnp.concatenate(shifted, axis=1)

    def relax(stage, x):
        if stage == 0:
            step = RELAX / first[nvar, x]
            step_of[x] = step
            step_edge[0, x : x + 1, :] = step[0:1]
            step_edge[1, x : x + 1, :] = step[ny - 1 : ny]
        else:
            step = step_of[x]
        total = None
        for k in range(nvar):
            value = (1.0 - RELAX) * field(stage)[k, x] + step * gathered(x, k)
            field(stage + 1)[k, x] = value
            keep_edges(edges.at[stage + 1], k, x, value)
            if stage == 0:
                keep_edges(row_true, k, x, value)
                for side, plane in ((0, 0), (1, nx - 1)):
                    if x == plane:
                        face_sent[side, k] = value
            if stage == 1:
                term = value * weight[k, x]
                total = term if k == 0 else total + term
        if stage == 1:
            surface[x] = total

    def settle(stage, x):
        for k in range(nvar):
            value = gathered(x, k) - first[nvar, x] * field(2)[k, x]
            residual_out[0, k, x] = value
            keep_edges(edges.at[3], k, x, value)

    def sweep(stage, finish):
        multiply(stage, 0)
        for x in range(nx):
            if x + 1 < nx:
                multiply(stage, x + 1)
            finish(stage, x)

    def brought(cells, d):
        out = []
        for k in range(nvar):
            total = flux[0, k, 0, d] * cells[0]
            for e in range(1, nvar):
                total = total + flux[e, k, 0, d] * cells[e]
            out.append(total)
        return out

    def halo_of(halo, more, stage, side):
        cells = [halo[stage, side, e] for e in range(nvar)]
        return [c + more[side, e] for e, c in enumerate(cells)] if stage == 1 else cells

    def begin_own():
        for side, d in ((0, 2), (1, 3)):
            mine = brought([edges[0, side, e] for e in range(nvar)], d)
            for k in range(nvar):
                row_more[side, k] = mine[k]
        for side, x, d in ((0, 0, 0), (1, nx - 1, 1)):
            mine = brought([first[e, x] for e in range(nvar)], d)
            for k in range(nvar):
                face_more[side, k] = mine[k]

    def add_corners():
        spot = lax.broadcasted_iota(jnp.int32, (8, nz), 0)
        lines_of = [corner[e] for e in range(nvar)]
        at_row = lax.broadcasted_iota(jnp.int32, (nx, nz), 0)
        at_face = lax.broadcasted_iota(jnp.int32, (ny, nz), 0)
        for k in range(nvar):
            along = []
            for near, ds in ((spot < 2, (1, 0)), (spot % 2 == 0, (3, 2))):
                total = None
                for e in range(nvar):
                    scale = jnp.where(near, flux[e, k, 0, ds[0]], flux[e, k, 0, ds[1]])
                    term = scale * lines_of[e]
                    total = term if e == 0 else total + term
                along.append(total)
            for side in range(2):
                ends = along[0][side : side + 1], along[0][2 + side : 3 + side]
                extra = jnp.where(at_row == 0, ends[0], jnp.where(at_row == nx - 1, ends[1], 0.0))
                row_more[side, k] = row_more[side, k] + extra
                ends = along[1][2 * side : 2 * side + 1], along[1][2 * side + 1 : 2 * side + 2]
                extra = jnp.where(at_face == 0, ends[0], jnp.where(at_face == ny - 1, ends[1], 0.0))
                face_more[side, k] = face_more[side, k] + extra

    def scale_more():
        for side, there in ((0, has_before_y), (1, has_after_y)):
            step = jnp.where(there, RELAX / row_halo[0, side, nvar], 0.0)
            for k in range(nvar):
                row_more[side, k] = step * row_more[side, k]
        for side, there in ((0, has_before_x), (1, has_after_x)):
            step = jnp.where(there, RELAX / face_halo[0, side, nvar], 0.0)
            for k in range(nvar):
                face_more[side, k] = step * face_more[side, k]

    def add_faces(stage):
        for side, x, d in ((0, 0, 1), (1, nx - 1, 0)):
            more = brought(halo_of(face_halo, face_more, stage, side), d)
            total = None
            for k in range(nvar):
                if stage == 2:
                    value = residual_out[0, k, x] + more[k]
                    residual_out[0, k, x] = value
                else:
                    part = step_of[x] * more[k]
                    value = field(stage + 1)[k, x] + part
                    field(stage + 1)[k, x] = value
                    if stage == 1:
                        term = part * weight[k, x]
                        total = term if k == 0 else total + term
                keep_edges(rows_of(stage + 1), k, x, value)
            if stage == 1:
                surface[x] = surface[x] + total

    def put_row(stage, k, y, value):
        for x in range(nx):
            if stage == 2:
                residual_out[0, k, x, y : y + 1, :] = value[x : x + 1]
            else:
                field(stage + 1)[k, x, y : y + 1, :] = value[x : x + 1]

    def add_rows(stage):
        for side, y, d in ((0, 0, 3), (1, ny - 1, 2)):
            more = brought(halo_of(row_halo, row_more, stage, side), d)
            total = None
            for k in range(nvar):
                part = more[k] if stage == 2 else step_edge[side] * more[k]
                value = rows_of(stage + 1)[side, k] + part
                if stage == 1:
                    edges[2, side, k] = value
                if stage == 1:
                    term = part * weight_edge[side, k]
                    total = term if k == 0 else total + term
                if stage != 1:
                    put_row(stage, k, y, value)
            if stage == 1:
                for x in range(nx):
                    surface[x, y : y + 1, :] = surface[x, y : y + 1, :] + total[x : x + 1]

    def complete(stage):
        faces, ranks = copies(stage)
        receive(faces)
        add_faces(stage)
        receive(ranks)
        add_rows(stage)

    for copy in source_loads:
        copy.wait()
    advance(0)
    sweep(0, relax)
    for plans in copies(1):
        begin(plans)
    begin_own()
    for copy in late_loads:
        copy.wait()
    for x in range(nx):
        cover = mask[x].astype(jnp.float32)
        for k in range(nvar):
            value = sensitivity[k, x].astype(jnp.float32) * cover
            weight[k, x] = value
            keep_edges(weight_edge, k, x, value)
    basis_parts[0], basis_parts[1] = split(basis[...])
    line = lax.broadcasted_iota(jnp.int32, (lines, nx * ny), 0)
    spots = jnp.concatenate([slots[x : x + 1, :] for x in range(nx)], axis=1)
    wanted = jnp.concatenate([2 * line, 2 * line + 1, 2 * line - 1], axis=0)
    onehot[...] = (wanted == spots).astype(jnp.float32).astype(jnp.bfloat16)
    for i in range(1, len(rounds) - 2):
        advance(i)
    complete(0)
    advance(len(rounds) - 2)
    receive(corner_copies)
    add_corners()
    sweep(1, relax)
    weight_sum = weights[0]
    for c in range(1, n_cond):
        weight_sum = weight_sum + weights[c]
    share = jnp.full((1, LANES), weights[ci], jnp.int32).astype(jnp.float32) / jnp.full(
        (1, LANES), weight_sum, jnp.int32
    ).astype(jnp.float32)
    receive(diagonal_copies())
    scale_more()

    complete(1)

    basis_high, basis_low = basis_parts[0], basis_parts[1]
    surface_high, surface_low = split(surface[...].reshape(nx * ny, nz))
    projected = (
        dot(surface_high, basis_high) + dot(surface_high, basis_low) + dot(surface_low, basis_high)
    )
    high, low = split(projected)
    looked = dot(onehot[...], high) + dot(onehot[...], low)
    turned = pltpu.roll(looked[lines:], LANES // 2, 1)
    spot = lax.broadcasted_iota(jnp.int32, (lines, LANES), 1)
    gradient = looked[:lines] + jnp.where(spot < LANES // 2, turned[lines:], turned[:lines])
    gradient = gradient * share
    for g in range(lines // rows):
        pieces[g] = gradient[g * rows : (g + 1) * rows]

    def group(gx, yz):
        return (gx * n_yz + yz) * per_owner // (rows * LANES)

    def give(c, gx, yz):
        remote(
            pieces.at[group(gx, yz)],
            arrived.at[me],
            (piece_sems.at[0], piece_sems.at[1]),
            (c, gx, yz),
        ).start()

    arrived[me] = pieces[group(xi, yi)]
    advance(len(rounds) - 1)
    if devices <= 64:
        turns = [(dc, dx, dy) for dc in range(n_cond) for dx in range(n_gx) for dy in range(n_yz)]
        ends = ((1, n_cond - 1), (1, n_gx - 1), (1, n_yz - 1))
        turns.sort(key=lambda t: -sum(d in e for d, e in zip(t, ends)))
        for dc, dx, dy in turns:
            if dc or dx or dy:
                give((ci + dc) % n_cond, (xi + dx) % n_gx, (yi + dy) % n_yz)
    else:

        def give_next(t, carry):
            flat = (me + t) % devices
            give(flat // (n_gx * n_yz), (flat // n_yz) % n_gx, flat % n_yz)
            return carry

        lax.fori_loop(1, devices, give_next, 0)

    for side, y in ((0, 0), (1, ny - 1)):
        for k in range(nvar):
            put_row(1, k, y, edges[2, side, k])
    for plans in copies(2):
        begin(plans)
    sweep(2, settle)
    complete(2)
    for stage in range(3):
        for plans in copies(stage):
            drain(plans)
    drain(corner_copies)
    drain(diagonal_copies())
    others = arrived.at[pl.ds(0, devices - 1)]
    for i in range(2):
        pltpu.make_async_copy(others, others, piece_sems.at[i]).wait()


def write(smoothed, residual, arrived, smoothed_hbm, residual_hbm, gradient_hbm, gradient, sems):
    stores = [
        pltpu.make_async_copy(src, dst, sems.at[i])
        for i, (src, dst) in enumerate(
            ((smoothed, smoothed_hbm), (residual, residual_hbm), (gradient, gradient_hbm))
        )
    ]
    for copy in stores[:2]:
        copy.start()
    gradient[...] = jnp.sum(arrived[...], axis=0)
    stores[2].start()
    for copy in stores:
        copy.wait()


def local(
    adjoint,
    objective_gradient,
    diagonal,
    flux_blocks,
    flux_sensitivity,
    surface_mask,
    patch_band_slot,
    design_basis,
    condition_weights,
):
    sizes = tuple(lax.axis_size(axis) for axis in ("cond", "gx", "yz"))
    devices = sizes[0] * sizes[1] * sizes[2]
    _, nvar, nx, ny, nz = adjoint.shape
    per_owner = NDES // (sizes[1] * sizes[2])
    rows = max(1, per_owner // LANES)
    lines = NDES // LANES
    rounds = max(len(spans_of(sizes[1])), len(spans_of(sizes[2]))) + 2
    f32 = jnp.float32
    hbm = pl.BlockSpec(memory_space=pltpu.MemorySpace.HBM)
    vmem = pl.BlockSpec(memory_space=pltpu.MemorySpace.VMEM)
    depth = -(-3 * nvar * ny // (2 * LANES)) * 2 * LANES
    grant = 67043328 - 2**16 - 2 * adjoint.size * 4 - 2**12 * devices
    smoothed, residual, arrived = pl.pallas_call(
        functools.partial(kernel, sizes),
        out_shape=(
            pltpu.VMEM(adjoint.shape, f32),
            pltpu.VMEM(adjoint.shape, f32),
            pltpu.VMEM((devices, rows, LANES), f32),
        ),
        in_specs=[hbm] * 9,
        out_specs=(vmem, vmem, vmem),
        scratch_shapes=[
            pltpu.VMEM((nvar + 1, nx, ny, nz), f32),
            pltpu.VMEM((nvar, nx, ny, nz), f32),
            pltpu.VMEM((nvar, nx, ny, nz), f32),
            pltpu.VMEM((nx, ny, nz), f32),
            pltpu.VMEM((5 * nvar * ny, depth), jnp.bfloat16),
            pltpu.VMEM((nx, depth, nz), jnp.bfloat16),
            pltpu.VMEM((nx, 5 * nvar * ny, nz), f32),
            pltpu.SMEM((nvar, nvar, 1, 6), f32),
            pltpu.VMEM((nvar, nx, ny, nz), jnp.bfloat16),
            pltpu.VMEM((nx, ny, nz), jnp.int32),
            pltpu.VMEM((nx, ny), jnp.int32),
            pltpu.VMEM(design_basis.shape, f32),
            pltpu.SMEM(condition_weights.shape, jnp.int32),
            pltpu.VMEM((nx, ny, nz), f32),
            pltpu.VMEM((4, 2, nvar + 1, nx, nz), f32),
            pltpu.VMEM((2, nvar, nx, nz), f32),
            pltpu.VMEM((2, nvar, ny, nz), f32),
            pltpu.VMEM((3, 2, nvar + 1, nx, nz), f32),
            pltpu.VMEM((3, 2, nvar + 1, ny, nz), f32),
            pltpu.VMEM((nvar, 8, nz), f32),
            pltpu.VMEM((2, nvar, nx, nz), f32),
            pltpu.VMEM((2, nvar, ny, nz), f32),
            pltpu.VMEM((2, nx, nz), f32),
            pltpu.VMEM((nvar, nx, ny, nz), f32),
            pltpu.VMEM((2, nvar, nx, nz), f32),
            pltpu.VMEM((2,) + design_basis.shape, jnp.bfloat16),
            pltpu.VMEM((3 * lines, nx * ny), jnp.bfloat16),
            pltpu.VMEM((NDES // (rows * LANES), rows, LANES), f32),
            pltpu.SemaphoreType.DMA((2,)),
            pltpu.SemaphoreType.DMA((4,)),
            pltpu.SemaphoreType.DMA((3,)),
            pltpu.SemaphoreType.DMA((3, 2, 2)),
            pltpu.SemaphoreType.DMA((3, 2, 2)),
            pltpu.SemaphoreType.DMA((2, 4)),
            pltpu.SemaphoreType.DMA((2, 4)),
            pltpu.SemaphoreType.DMA((2,)),
            pltpu.SemaphoreType.REGULAR((rounds,)),
        ],
        compiler_params=pltpu.CompilerParams(
            collective_id=0, has_side_effects=True, vmem_limit_bytes=grant
        ),
    )(
        adjoint,
        objective_gradient,
        diagonal,
        jnp.transpose(flux_blocks, (2, 3, 0, 1)),
        flux_sensitivity,
        surface_mask,
        patch_band_slot,
        design_basis,
        condition_weights,
    )
    smoothed, residual, gradient = pl.pallas_call(
        write,
        out_shape=(
            jax.ShapeDtypeStruct(adjoint.shape, f32),
            jax.ShapeDtypeStruct(adjoint.shape, f32),
            jax.ShapeDtypeStruct((rows, LANES), f32),
        ),
        in_specs=[vmem] * 3,
        out_specs=(hbm, hbm, hbm),
        scratch_shapes=[pltpu.VMEM((rows, LANES), f32), pltpu.SemaphoreType.DMA((3,))],
        compiler_params=pltpu.CompilerParams(vmem_limit_bytes=2**20),
    )(smoothed, residual, arrived)
    flat = gradient.reshape(-1)
    if per_owner < flat.shape[0]:
        owner = lax.axis_index(("gx", "yz"))
        flat = lax.dynamic_slice_in_dim(flat, (owner * per_owner) % flat.shape[0], per_owner, 0)
    return smoothed, residual, flat


def solution(mesh):
    placed = (
        P("cond", None, "gx", "yz", None),
        P("cond", None, "gx", "yz", None),
        P("gx", "yz", None),
        P("cond", None, None, None),
        P("cond", None, "gx", "yz", None),
        P("gx", "yz", None),
        P("gx", "yz"),
        P(),
        P(),
    )
    return jax.shard_map(
        local,
        mesh=mesh,
        in_specs=placed,
        out_specs=(
            P("cond", None, "gx", "yz", None),
            P("cond", None, "gx", "yz", None),
            P(("gx", "yz")),
        ),
        check_vma=False,
    )
```
